32 devices in a mesh: dom: 8 (over y, x, core), feat: 4 (over z).
Axes of the slice: x: 2, y: 2, z: 4, core: 2. Of those that a mesh axis runs over, the one named last changes fastest.
Arguments:
- features: bfloat16 [128, 131072], P('feat', 'dom'), may hold values from -6 to 6
- seed_rows: int32 [2048], P('dom'), may hold values from 0 to 16383
- want_rows: int32 [8, 8, 128], P('dom'), may hold values from 0 to 16383
- live_counts: int32 [8, 8], P('dom'), may hold values from 1 to 128, as said below
- hop_one: int32 [15, 2048], P(None, 'dom'), may hold values from 0 to 1023, as said below
- hop_two: int32 [10, 15, 2048], P(None, None, 'dom'), may hold values from 0 to 1023, as said below
- w1_self: bfloat16 [256, 128], replicated, may hold values from -0.5 to 0.5
- w1_neigh: bfloat16 [256, 128], replicated, may hold values from -0.5 to 0.5
- b1: float32 [256], P('feat'), may hold values from -4 to 4
- w2_self: bfloat16 [256, 256], P(None, 'feat'), may hold values from -0.375 to 0.375
- w2_neigh: bfloat16 [256, 256], P(None, 'feat'), may hold values from -0.375 to 0.375
- b2: float32 [256], P('feat'), may hold values from -4 to 4
Outputs:
- embed: float32 [256, 2048], P('feat', 'dom')
The draws below stay inside these ranges and needn't reach their ends.
Inputs may be any that keep to these rules, and one draw needn't show every extreme that they name: `want_rows`: slots at or beyond live_counts[r, o] are ignored. `live_counts`: in every draw a quarter of the owners, every fourth one from a drawn offset, receive all 128 slots from every requester. `hop_one`: each entry is o * 128 + c, a position in the buffer of the requester that holds seed s, with c < live_counts of that requester and owner o. `hop_two`: each entry is o * 128 + c, a position in the buffer of the requester that holds seed s, with c < live_counts of that requester and owner o.
All inputs are finite; a program needn't handle non-finite values.
Results may differ from the reference program's by a relative error of at most 0.00036.
Values may be sent and summed in bfloat16 or wider, within the bound.
A program may use at most 64 MiB of HBM per device.

```python
import jax
import jax.numpy as jnp
from jax import lax

FEAT = 128
HID = 256
OUT = 256
FAN1 = 15
FAN2 = 10
CAP = 128
SEED_DEV = 256
NODE_DEV = 16384
OWNERS = 8
SEEDS = 2048
NODES = 131072


def slot_plan(key):
    offset = jax.random.randint(jax.random.fold_in(key, 501), (), 0, 4)
    owner = jnp.arange(OWNERS, dtype=jnp.int32)
    spread = jax.random.randint(jax.random.fold_in(key, 502), (OWNERS, OWNERS), CAP // 8, CAP + 1)
    full = ((owner - offset) % 4 == 0)[None, :]
    return (offset, jnp.where(full, CAP, spread).astype(jnp.int32))


def positions(key, salt, lead):
    offset, counts = slot_plan(key)
    draw_key = jax.random.fold_in(key, salt)
    shape = lead + (SEEDS,)
    requester = jnp.broadcast_to(jnp.arange(SEEDS, dtype=jnp.int32) // SEED_DEV, shape)
    choose = jax.random.randint(jax.random.fold_in(draw_key, 1), shape, 0, 2)
    favored = (offset + 4 * jax.random.randint(jax.random.fold_in(draw_key, 2), shape, 0, OWNERS // 4)) % OWNERS
    anyone = jax.random.randint(jax.random.fold_in(draw_key, 3), shape, 0, OWNERS)
    owner = jnp.where(choose == 1, favored, anyone).astype(jnp.int32)
    limit = counts[requester, owner]
    slot = jax.random.randint(jax.random.fold_in(draw_key, 4), shape, 0, 1 << 20) % limit
    return (owner * CAP + slot).astype(jnp.int32)


def draw_live_counts(key, part):
    return slot_plan(key)[1]


def draw_hop_one(key, part):
    return positions(key, 11, (FAN1,))


def draw_hop_two(key, part):
    return positions(key, 12, (FAN2, FAN1))


def plant(values, stream_key, least, top_value):
    spot = [jax.random.randint(jax.random.fold_in(stream_key, axis), (), 0, length) for axis, length in enumerate(values.shape)]
    widest = values.shape.index(max(values.shape))
    neighbour = spot[:widest] + [(spot[widest] + 1) % values.shape[widest]] + spot[widest + 1:]
    return values.at[tuple(spot)].set(least).at[tuple(neighbour)].set(top_value)


def block_levels(rng, dims, cuts, least, top_value):
    gain = 1.0
    for axis_at, blocks in cuts:
        steps = jax.random.uniform(jax.random.fold_in(jax.random.fold_in(rng, 6), axis_at), (blocks,), jnp.float32, least / len(cuts), top_value / len(cuts))
        gain = gain * jnp.repeat(jnp.exp(steps), dims[axis_at] // blocks).reshape((-1,) + (1,) * (len(dims) - 1 - axis_at))
    return gain


def centred(own_key, dims, scale, most, pieces=(), kind=jnp.bfloat16):
    level = block_levels(own_key, dims, pieces, -0.22, 0.18) if pieces else 1.0
    entries = jax.random.normal(own_key, dims, jnp.float32) * scale * level
    return jnp.minimum(jnp.maximum(entries, -most), most).astype(kind)


def setup_inputs(seed: int = 0) -> dict:
    arg_keys = jax.random.split(jax.random.key(seed), 13)
    features = centred(arg_keys[0], (FEAT, NODES), 1.0, 6.0, ((0, 4), (1, 8)))
    seed_rows = plant(jax.random.randint(arg_keys[1], (SEEDS,), 0, NODE_DEV), jax.random.fold_in(arg_keys[1], 1), 0, NODE_DEV - 1).astype(jnp.int32)
    want_rows = plant(jax.random.randint(arg_keys[2], (OWNERS, OWNERS, CAP), 0, NODE_DEV), jax.random.fold_in(arg_keys[2], 1), 0, NODE_DEV - 1).astype(jnp.int32)
    live_counts = draw_live_counts(jax.random.fold_in(arg_keys[12], 71), 0)
    hop_one = draw_hop_one(jax.random.fold_in(arg_keys[12], 71), 0)
    hop_two = draw_hop_two(jax.random.fold_in(arg_keys[12], 71), 0)
    w1_self = centred(arg_keys[6], (HID, FEAT), FEAT ** -0.5, 0.5)
    w1_neigh = centred(arg_keys[7], (HID, FEAT), FEAT ** -0.5, 0.5)
    b1 = centred(arg_keys[8], (HID,), 1.0, 4.0, ((0, 4),), jnp.float32)
    w2_self = centred(arg_keys[9], (OUT, HID), HID ** -0.5, 0.375, ((1, 4),))
    w2_neigh = centred(arg_keys[10], (OUT, HID), HID ** -0.5, 0.375, ((1, 4),))
    b2 = centred(arg_keys[11], (OUT,), 1.0, 4.0, ((0, 4),), jnp.float32)
    return {"features": features, "seed_rows": seed_rows, "want_rows": want_rows, "live_counts": live_counts, "hop_one": hop_one, "hop_two": hop_two, "w1_self": w1_self, "w1_neigh": w1_neigh, "b1": b1, "w2_self": w2_self, "w2_neigh": w2_neigh, "b2": b2}


def reference(features, seed_rows, want_rows, live_counts, hop_one, hop_two, w1_self, w1_neigh, b1, w2_self, w2_neigh, b2):
    owner = jnp.arange(OWNERS, dtype=jnp.int32)
    nodes = want_rows + (owner * NODE_DEV)[None, :, None]
    fetched = jnp.take(features, nodes.reshape(-1).astype(jnp.int32), axis=1)
    slot = jnp.arange(CAP, dtype=jnp.int32)
    live = slot[None, None, :] < live_counts[:, :, None]
    fetched = jnp.where(live.reshape(1, -1), fetched, jnp.zeros((), fetched.dtype))
    requester = jnp.arange(SEEDS, dtype=jnp.int32) // SEED_DEV
    base = requester * (OWNERS * CAP)
    x_one = jnp.take(fetched, (hop_one + base[None, :]).reshape(-1).astype(jnp.int32), axis=1)

    def add_hop(number, total):
        picked = jnp.take(fetched, (hop_two[number] + base[None, :]).reshape(-1).astype(jnp.int32), axis=1)
        return total + picked.astype(jnp.float32)
    m_two = lax.fori_loop(0, FAN2, add_hop, jnp.zeros((FEAT, FAN1 * SEEDS), jnp.float32))
    m_two = (m_two * (1.0 / FAN2)).astype(jnp.bfloat16)
    x_seed = jnp.take(features, (seed_rows + requester * NODE_DEV).astype(jnp.int32), axis=1)
    m_one = (lax.optimization_barrier(jnp.sum(x_one.reshape(FEAT, FAN1, SEEDS).astype(jnp.float32), axis=1)) * (1.0 / FAN1)).astype(jnp.bfloat16)

    def layer(selves, means):
        pre = jnp.dot(w1_self, selves, preferred_element_type=jnp.float32)
        pre = pre + jnp.dot(w1_neigh, means, preferred_element_type=jnp.float32) + b1[:, None]
        return jnp.maximum(pre, 0.0)
    h_one = layer(x_one, m_two)
    h_seed = layer(x_seed, m_one)
    g_mean = lax.optimization_barrier(jnp.sum(h_one.reshape(HID, FAN1, SEEDS), axis=1)) * (1.0 / FAN1)
    z_out = jnp.dot(w2_self.astype(jnp.float32), h_seed, precision=lax.Precision.HIGHEST, preferred_element_type=jnp.float32)
    z_out = z_out + jnp.dot(w2_neigh.astype(jnp.float32), g_mean, precision=lax.Precision.HIGHEST, preferred_element_type=jnp.float32) + b2[:, None]
    square = lax.optimization_barrier(jnp.sum(z_out * z_out, axis=0))
    return z_out * lax.rsqrt(square * (1.0 / OUT) + 1.0)
```

```python
import functools

import jax
import jax.numpy as jnp
from jax import lax
from jax.experimental import pallas as pl
from jax.experimental.pallas import tpu as pltpu
from jax.sharding import PartitionSpec as P

LANES = 128
MESH = pl.DeviceIdType.MESH
BF16 = jnp.bfloat16
F32 = jnp.float32


def split_three(x):
    a = x.astype(BF16)
    rest = x - a.astype(F32)
    b = rest.astype(BF16)
    c = (rest - b.astype(F32)).astype(BF16)
    return a, b, c


def kernel(
    nd,
    nf,
    feat_hbm,
    seed_hbm,
    want_hbm,
    live_hbm,
    one_hbm,
    two_hbm,
    w1s_hbm,
    w1n_hbm,
    w2s_hbm,
    w2n_hbm,
    b1_hbm,
    b2_hbm,
    out_ref,
    feat_vm,
    seed_vm,
    seed_sm,
    want_vm,
    live_sm,
    one_ref,
    two_ref,
    w1s_ref,
    w1n_ref,
    ask,
    got,
    got_sm,
    table,
    rows_vm,
    served,
    everyone,
    seed_own,
    seed_all,
    w2_all,
    b1_all,
    b2_all,
    hop_rows,
    words,
    pick_one,
    pick_two,
    own_sum,
    mean_sum,
    x_all,
    m_all,
    w2_full,
    z_own,
    z_all,
    local_sem,
    ready,
    want_send,
    want_recv,
    want_sm_send,
    want_sm_recv,
    data_send,
    data_recv,
    seed_send,
    seed_recv,
    early_send,
    early_recv,
    z_send,
    z_recv,
):
    height, nodes = feat_vm.shape
    fan1, seeds = one_ref.shape
    fan2 = two_ref.shape[0]
    sub = seeds // nf
    per = LANES // sub
    chunks = (fan1 + 1) * sub // LANES
    hid_dev = out_ref.shape[0]
    hid = w1s_ref.shape[0]
    depth = w1s_ref.shape[1]
    groups = seeds // LANES
    pieces = depth // height
    table_rows = nodes // pieces
    me = lax.axis_index("dom")
    mf = lax.axis_index("feat")

    def dom_at(d):
        return lax.rem(me + d, nd)

    def feat_at(d):
        return lax.rem(mf + d, nf)

    def local(i, src, dst):
        copy = pltpu.make_async_copy(src, dst, local_sem.at[i])
        copy.start()
        return copy

    barrier = pltpu.get_barrier_semaphore()
    for d in range(1, nf):
        pl.semaphore_signal(barrier, inc=1, device_id={"feat": feat_at(d)}, device_id_type=MESH)
    for d in range(1, nd):
        pl.semaphore_signal(barrier, inc=1, device_id={"dom": dom_at(d)}, device_id_type=MESH)

    want_copies = [local(0, want_hbm.at[0], want_vm), local(1, live_hbm, live_sm)]
    feat_copy = local(2, feat_hbm, feat_vm)
    early_copies = [
        local(3, w2s_hbm, w2_all.at[0, mf]),
        local(4, w2n_hbm, w2_all.at[1, mf]),
        local(5, b1_hbm, b1_all.at[mf]),
        local(6, b2_hbm, b2_all.at[mf]),
    ]
    seed_local = [local(7, seed_hbm, seed_vm), local(8, seed_hbm, seed_sm)]
    hop_copies = [local(9, one_hbm, one_ref), local(10, two_hbm, two_ref)]
    weight_copies = [local(11, w1s_hbm, w1s_ref), local(12, w1n_hbm, w1n_ref)]

    def remote(src, dst, send, recv, where):
        copy = pltpu.make_async_remote_copy(
            src_ref=src,
            dst_ref=dst,
            send_sem=send,
            recv_sem=recv,
            device_id=where,
            device_id_type=MESH,
        )
        copy.start()
        return copy

    lane = lax.broadcasted_iota(jnp.int32, (1, LANES), 1)
    for copy in want_copies:
        copy.wait()
    for o in range(nd):
        ask[o] = jnp.where(lane < live_sm[0, o], want_vm[o : o + 1], -1)
    pl.semaphore_wait(barrier, nd + nf - 2)

    wants = []
    for d in range(1, nd):
        pl.semaphore_signal(ready, inc=1, device_id={"dom": dom_at(d)}, device_id_type=MESH)
    for d in range(1, nd):
        where = {"dom": dom_at(d)}
        src = ask.at[dom_at(d)]
        wants.append(remote(src, got_sm.at[d], want_sm_send.at[d], want_sm_recv.at[d], where))
        wants.append(remote(src, got.at[d], want_send.at[d], want_recv.at[d], where))
    own_sm = local(13, ask.at[me], got_sm.at[0])
    got[0] = ask[me]
    for copy in early_copies:
        copy.wait()
    early = []
    for d in range(1, nf):
        where = {"feat": feat_at(d)}
        for i, ref in enumerate(
            (b1_all.at[mf], b2_all.at[mf], w2_all.at[0, mf], w2_all.at[1, mf])
        ):
            early.append(remote(ref, ref, early_send.at[d, i], early_recv.at[d, i], where))

    feat_copy.wait()
    tiles = table_rows // LANES
    step = min(8, tiles)

    def turn(i, carry):
        for u in range(step):
            t = i * step + u
            stack = jnp.concatenate(
                [
                    feat_vm[
                        :, pl.ds(pl.multiple_of(p * table_rows + t * LANES, LANES), LANES)
                    ].astype(F32)
                    for p in range(pieces)
                ],
                axis=0,
            )
            table[pl.ds(pl.multiple_of(t * LANES, LANES), LANES), :] = jnp.transpose(stack)
        return carry

    lax.fori_loop(0, tiles // step, turn, 0)

    def gather(slot, read, wanted):
        burst = 32

        def body(i, carry):
            for u in range(burst):
                k = i * burst + u
                row = read(k) & (table_rows - 1)
                rows_vm[slot, pl.ds(k, 1), :] = table[pl.ds(row, 1), :]
            return carry

        lax.fori_loop(0, LANES // burst, body, 0)
        turned = jnp.transpose(rows_vm[slot])
        piece = wanted >> (table_rows.bit_length() - 1)
        block = jnp.zeros((height, LANES), F32)
        for p in range(pieces):
            block = jnp.where(piece == p, turned[p * height : (p + 1) * height], block)
        return block.astype(BF16)

    for copy in seed_local:
        copy.wait()
    for g in range(groups):
        seed_own[g] = gather(
            nd + g,
            lambda k: seed_sm[0, g * LANES + k],
            seed_vm[:, g * LANES : (g + 1) * LANES],
        )
    seed_copies = [
        remote(
            seed_own.at[feat_at(d) * sub // LANES],
            seed_all.at[mf],
            seed_send.at[d],
            seed_recv.at[d],
            {"feat": feat_at(d)},
        )
        for d in range(1, nf)
    ]
    seed_all[mf] = seed_own[mf * sub // LANES]

    order = list(range(1, nd)) + [0]
    parts = [order[: nd * 3 // 8], order[nd * 3 // 8 : nd * 6 // 8], order[nd * 6 // 8 :]]
    data = {}
    pl.semaphore_wait(ready, nd - 1)
    for d in order:
        if d:
            wants[2 * d - 2].wait_recv()
            wants[2 * d - 1].wait_recv()
        else:
            own_sm.wait()
        served[d] = gather(d, lambda k: got_sm[d, 0, k], got[d])
        for e in range(nf - 1, -1, -1):
            where = {"dom": dom_at(nd - d), "feat": feat_at(e)}
            if d or e:
                data[d, e] = remote(
                    served.at[d],
                    everyone.at[d, mf],
                    data_send.at[d, e],
                    data_recv.at[d, e],
                    where,
                )
        if d == 0:
            everyone[0, mf] = served[0]

    base = pl.multiple_of(mf * sub // LANES * LANES, LANES)
    within = lax.rem(mf * sub, LANES)
    for copy in hop_copies:
        copy.wait()
    for k in range(fan2 + 1):
        if k < fan2:
            rows = two_ref[k, :, pl.ds(base, LANES)]
        else:
            rows = one_ref[:, pl.ds(base, LANES)]
        rel = (rows >> 7) - me - 1
        rows = (rows & (LANES - 1)) + jnp.where(rel < 0, rel + nd, rel) * LANES
        turned = [
            pltpu.roll(rows, lax.rem(q * sub - within + LANES, LANES), 1) for q in range(per)
        ]
        for c in range(chunks):
            row = jnp.full((1, LANES), -1, jnp.int32)
            for q in range(per):
                j = c * per + q
                if j < fan1:
                    inside = (lane >= q * sub) & (lane < (q + 1) * sub)
                    row = jnp.where(inside, turned[q][j : j + 1], row)
            hop_rows[c, k : k + 1, :] = row

    slot = lax.broadcasted_iota(jnp.int32, (LANES, LANES), 0)
    each = 8
    for c in range(chunks):
        columns = slice(c * LANES, (c + 1) * LANES)
        for g in range(words.shape[0]):
            count = jnp.zeros((LANES, LANES), jnp.int32)
            for k in range(fan2):
                row = hop_rows[c, k : k + 1, :]
                rel = (row >> 7) - g * each
                real = (row >= 0) & (rel >= 0) & (rel < each)
                unit = jnp.where(real, jnp.left_shift(1, (rel & (each - 1)) * 4), 0)
                count = count + jnp.where((row & (LANES - 1)) == slot, unit, 0)
            words[g, :, columns] = count

    def build(o, carry):
        start = pl.multiple_of(o * LANES, LANES)
        place = slot + o * LANES
        shift = lax.rem(o, each) * 4
        for c in range(chunks):
            columns = slice(c * LANES, (c + 1) * LANES)
            count = lax.shift_right_logical(words[o // each, :, columns], shift) & 15
            pick_two[pl.ds(start, LANES), columns] = count.astype(F32).astype(BF16)
            pick_one[pl.ds(start, LANES), columns] = jnp.where(
                hop_rows[c, fan2 : fan2 + 1, :] == place, 1.0, 0.0
            ).astype(BF16)
        return carry

    lax.fori_loop(0, nd, build, 0)

    for copy in early:
        copy.wait_recv()
    for copy in weight_copies:
        copy.wait()
    w2_full[...] = jnp.transpose(w2_all[...].reshape(2 * hid, w2_all.shape[3]))

    def column(rows):
        return jnp.concatenate(
            [jnp.transpose(jnp.broadcast_to(rows[f], (LANES, hid_dev))) for f in range(nf)], axis=0
        )

    b1 = column(b1_all)
    b2 = column(b2_all)
    for copy in seed_copies:
        copy.wait_recv()

    def whole(blocks):
        if height % 16:
            return blocks.astype(F32).reshape(depth, LANES).astype(BF16)
        return blocks.reshape(depth, LANES)

    x_seed = whole(seed_all[...]).astype(F32)
    x_seed = pltpu.roll(x_seed, lax.rem(2 * LANES - sub - within, LANES), 1)

    wide = 2 * LANES
    total = jnp.zeros((depth, LANES), F32)
    done = 0
    for i, part in enumerate(parts):
        for d in part:
            for e in range(nf):
                if d or e:
                    data[d, e].wait_recv()
        fetched = jnp.concatenate([whole(everyone[d]) for d in part], axis=1)
        these = slice(done, done + len(part) * LANES)
        done += len(part) * LANES
        for n in range(chunks * LANES // wide):
            columns = slice(n * wide, (n + 1) * wide)
            own = jnp.dot(fetched, pick_one[these, columns], preferred_element_type=F32)
            mean = jnp.dot(fetched, pick_two[these, columns], preferred_element_type=F32)
            if i:
                own = own + own_sum[:, columns]
                mean = mean + mean_sum[:, columns]
            if i < len(parts) - 1:
                own_sum[:, columns] = own
                mean_sum[:, columns] = mean
                continue
            total = total + own[:, :LANES] + own[:, LANES:]
            x_all[:, columns] = own.astype(BF16)
            m_all[:, columns] = (mean * (1.0 / fan2)).astype(BF16)

    def fold(value):
        width = sub
        while width < LANES:
            value = value + pltpu.roll(value, width, 1)
            width *= 2
        return value

    is_seed = lane >= LANES - sub
    last = slice((chunks - 1) * LANES, chunks * LANES)
    m_one = fold(total) * (1.0 / fan1)
    x_all[:, last] = jnp.where(is_seed, x_seed, x_all[:, last].astype(F32)).astype(BF16)
    m_all[:, last] = jnp.where(is_seed, m_one, m_all[:, last].astype(F32)).astype(BF16)

    total = jnp.zeros((hid, LANES), F32)
    for n in range(chunks * LANES // wide):
        columns = slice(n * wide, (n + 1) * wide)
        pre = jnp.dot(w1s_ref[...], x_all[:, columns], preferred_element_type=F32)
        pre = pre + jnp.dot(w1n_ref[...], m_all[:, columns], preferred_element_type=F32)
        left = jnp.maximum(pre[:, :LANES] + b1, 0.0)
        right = jnp.maximum(pre[:, LANES:] + b1, 0.0)
        if n == chunks * LANES // wide - 1:
            h_seed = right
            right = jnp.where(is_seed, 0.0, right)
        total = total + left + right
    g_mean = fold(total) * (1.0 / fan1)
    stacked = jnp.concatenate([h_seed, g_mean], axis=0)
    z = jnp.zeros((hid, LANES), F32)
    for term in reversed(split_three(stacked)):
        z = z + jnp.dot(w2_full[...], term, preferred_element_type=F32)
    z = z + b2
    square = jnp.sum(z * z, axis=0, keepdims=True)
    z = z * lax.rsqrt(square * (1.0 / hid) + 1.0)
    part_rows = hid_dev // per
    for f in range(nf):
        packed = jnp.zeros((part_rows, LANES), F32)
        for p in range(per):
            row = f * hid_dev + p * part_rows
            value = z[row : row + part_rows]
            shift = (p * sub + sub) % LANES
            if shift:
                value = pltpu.roll(value, shift, 1)
            packed = jnp.where((lane >= p * sub) & (lane < (p + 1) * sub), value, packed)
        z_own[f] = packed

    z_copies = [
        remote(
            z_own.at[feat_at(d)],
            z_all.at[mf],
            z_send.at[d],
            z_recv.at[d],
            {"feat": feat_at(d)},
        )
        for d in range(1, nf)
    ]
    z_all[mf] = z_own[mf]
    for copy in wants + early + seed_copies + list(data.values()):
        copy.wait_send()
    for copy in z_copies:
        copy.wait_recv()
    for g in range(groups):
        for p in range(per):
            block = jnp.zeros((part_rows, LANES), F32)
            for q in range(per):
                value = z_all[g * per + q]
                shift = (q - p) * sub % LANES
                if shift:
                    value = pltpu.roll(value, shift, 1)
                inside = (lane >= q * sub) & (lane < (q + 1) * sub)
                block = jnp.where(inside, value, block)
            out_ref[p * part_rows : (p + 1) * part_rows, g * LANES : (g + 1) * LANES] = block
    for copy in z_copies:
        copy.wait_send()


def per_device(
    nd,
    nf,
    features,
    seed_rows,
    want_rows,
    live_counts,
    hop_one,
    hop_two,
    w1_self,
    w1_neigh,
    b1,
    w2_self,
    w2_neigh,
    b2,
):
    height, nodes = features.shape
    seeds = seed_rows.shape[0]
    hid_dev = b1.shape[0]
    hid, depth = w1_self.shape
    cap = want_rows.shape[2]
    fan1 = hop_one.shape[0]
    columns = (fan1 + 1) * (seeds // nf)
    groups = seeds // LANES
    vmem = pl.BlockSpec(memory_space=pltpu.VMEM)
    dma = pltpu.SemaphoreType.DMA
    return pl.pallas_call(
        functools.partial(kernel, nd, nf),
        out_shape=pltpu.VMEM((hid_dev, seeds), F32),
        in_specs=[pl.BlockSpec(memory_space=pl.ANY)] * 12,
        out_specs=vmem,
        scratch_shapes=[
            pltpu.VMEM((height, nodes), BF16),
            pltpu.VMEM((1, seeds), jnp.int32),
            pltpu.SMEM((1, seeds), jnp.int32),
            pltpu.VMEM((nd, cap), jnp.int32),
            pltpu.SMEM((1, nd), jnp.int32),
            pltpu.VMEM(hop_one.shape, jnp.int32),
            pltpu.VMEM(hop_two.shape, jnp.int32),
            pltpu.VMEM(w1_self.shape, BF16),
            pltpu.VMEM(w1_neigh.shape, BF16),
            pltpu.VMEM((nd, 1, cap), jnp.int32),
            pltpu.VMEM((nd, 1, cap), jnp.int32),
            pltpu.SMEM((nd, 1, cap), jnp.int32),
            pltpu.VMEM((nodes * height // depth, LANES), F32),
            pltpu.VMEM((nd + groups, LANES, LANES), F32),
            pltpu.VMEM((nd, height, cap), BF16),
            pltpu.VMEM((nd, nf, height, cap), BF16),
            pltpu.VMEM((groups, height, LANES), BF16),
            pltpu.VMEM((nf, height, LANES), BF16),
            pltpu.VMEM((2, nf, hid_dev, w2_self.shape[0]), BF16),
            pltpu.VMEM((nf, 1, hid_dev), F32),
            pltpu.VMEM((nf, 1, hid_dev), F32),
            pltpu.VMEM((columns // LANES, 16, LANES), jnp.int32),
            pltpu.VMEM((pl.cdiv(nd, 8), LANES, columns), jnp.int32),
            pltpu.VMEM((nd * cap, columns), BF16),
            pltpu.VMEM((nd * cap, columns), BF16),
            pltpu.VMEM((depth, columns), F32),
            pltpu.VMEM((depth, columns), F32),
            pltpu.VMEM((depth, columns), BF16),
            pltpu.VMEM((depth, columns), BF16),
            pltpu.VMEM((hid, 2 * hid), BF16),
            pltpu.VMEM((nf, hid_dev * (seeds // nf) // LANES, LANES), F32),
            pltpu.VMEM((nf, hid_dev * (seeds // nf) // LANES, LANES), F32),
            dma((14,)),
            pltpu.SemaphoreType.REGULAR,
        ]
        + [dma((nd,))] * 4
        + [dma((nd, nf))] * 2
        + [dma((nf,))] * 2
        + [dma((nf, 4))] * 2
        + [dma((nf,))] * 2,
        compiler_params=pltpu.CompilerParams(collective_id=0, has_side_effects=True),
    )(
        features,
        seed_rows.reshape(1, seeds),
        want_rows,
        live_counts,
        hop_one,
        hop_two,
        w1_self,
        w1_neigh,
        w2_self.T,
        w2_neigh.T,
        b1.reshape(1, hid_dev),
        b2.reshape(1, hid_dev),
    )


def solution(mesh):
    return jax.shard_map(
        functools.partial(per_device, mesh.shape["dom"], mesh.shape["feat"]),
        mesh=mesh,
        in_specs=(
            P("feat", "dom"),
            P("dom"),
            P("dom", None, None),
            P("dom", None),
            P(None, "dom"),
            P(None, None, "dom"),
            P(),
            P(),
            P("feat"),
            P(None, "feat"),
            P(None, "feat"),
            P("feat"),
        ),
        out_specs=P("feat", "dom"),
        check_vma=False,
    )
```

```python
import functools

import jax
import jax.numpy as jnp
from jax import lax
from jax.experimental import pallas as pl
from jax.experimental.pallas import tpu as pltpu
from jax.sharding import PartitionSpec as P

LANES = 128
MESH = pl.DeviceIdType.MESH
BF16 = jnp.bfloat16
F32 = jnp.float32


def split_three(x):
    a = x.astype(BF16)
    rest = x - a.astype(F32)
    b = rest.astype(BF16)
    c = (rest - b.astype(F32)).astype(BF16)
    return a, b, c


def kernel(
    nd,
    nf,
    feat_hbm,
    seed_hbm,
    want_hbm,
    live_hbm,
    one_hbm,
    two_hbm,
    w1s_hbm,
    w1n_hbm,
    w2s_hbm,
    w2n_hbm,
    b1_hbm,
    b2_hbm,
    out_ref,
    feat_vm,
    seed_vm,
    seed_sm,
    want_vm,
    live_sm,
    one_ref,
    two_ref,
    w1s_ref,
    w1n_ref,
    ask,
    got,
    got_sm,
    table,
    rows_vm,
    served,
    everyone,
    seed_own,
    seed_all,
    w2_all,
    b1_all,
    b2_all,
    hop_rows,
    words,
    pick_one,
    pick_two,
    own_sum,
    mean_sum,
    x_all,
    m_all,
    w2_full,
    z_own,
    z_all,
    local_sem,
    ready,
    want_send,
    want_recv,
    want_sm_send,
    want_sm_recv,
    data_send,
    data_recv,
    seed_send,
    seed_recv,
    early_send,
    early_recv,
    pair_send,
    pair_recv,
    pass_send,
    pass_recv,
    z_send,
    z_recv,
):
    height, nodes = feat_vm.shape
    _, fan1, seeds = one_ref.shape
    fan2 = two_ref.shape[1]
    sub = seeds // nf
    per = LANES // sub
    chunks = (fan1 + 1) * sub // LANES
    hid_dev = out_ref.shape[0]
    hid = w1s_ref.shape[0]
    depth = w1s_ref.shape[1]
    groups = seeds // LANES
    pieces = depth // height
    table_rows = nodes // pieces
    me = lax.axis_index("dom")
    mf = lax.axis_index("feat")
    pairs = nd // 2
    half = nf // 2
    odd = lax.rem(me, 2)
    late = mf // half
    home = odd == late
    worker = odd * half + lax.rem(mf, half)

    def flip(x, bits):
        bit = 1
        while bit <= bits:
            if bits & bit:
                x = x + bit * (1 - 2 * lax.rem(x // bit, 2))
            bit *= 2
        return x

    def other(t):
        return odd + t * (1 - 2 * odd)

    def dom_at(d, t):
        return 2 * flip(me // 2, d) + other(t)

    def feat_at(d):
        return lax.rem(mf + d, nf)

    def local(i, src, dst):
        copy = pltpu.make_async_copy(src, dst, local_sem.at[i])
        copy.start()
        return copy

    barrier = pltpu.get_barrier_semaphore()
    for d in range(1, nf):
        pl.semaphore_signal(barrier, inc=1, device_id={"feat": feat_at(d)}, device_id_type=MESH)
    peers = [(d, t) for d in range(pairs) for t in range(2)][1:]
    for d, t in peers:
        pl.semaphore_signal(barrier, inc=1, device_id={"dom": dom_at(d, t)}, device_id_type=MESH)

    want_copies = [local(0, want_hbm.at[0], want_vm), local(1, live_hbm, live_sm)]
    feat_copy = local(2, feat_hbm, feat_vm)
    early_copies = [
        local(3, w2s_hbm, w2_all.at[0, mf]),
        local(4, w2n_hbm, w2_all.at[1, mf]),
        local(5, b1_hbm, b1_all.at[mf]),
        local(6, b2_hbm, b2_all.at[mf]),
    ]
    seed_local = [local(7, seed_hbm, seed_vm), local(8, seed_hbm, seed_sm)]
    hop_copies = [local(9, one_hbm, one_ref.at[0]), local(10, two_hbm, two_ref.at[0])]
    weight_copies = [local(11, w1s_hbm, w1s_ref), local(12, w1n_hbm, w1n_ref)]

    def remote(src, dst, send, recv, where):
        copy = pltpu.make_async_remote_copy(
            src_ref=src,
            dst_ref=dst,
            send_sem=send,
            recv_sem=recv,
            device_id=where,
            device_id_type=MESH,
        )
        copy.start()
        return copy

    lane = lax.broadcasted_iota(jnp.int32, (1, LANES), 1)
    for copy in want_copies:
        copy.wait()
    for o in range(nd):
        ask[o] = jnp.where(lane < live_sm[0, o], want_vm[o : o + 1], -1)
    pl.semaphore_wait(barrier, nd + nf - 2)

    for d, t in peers:
        pl.semaphore_signal(ready, inc=1, device_id={"dom": dom_at(d, t)}, device_id_type=MESH)
    wants = {}
    for d, t in peers:
        where = {"dom": dom_at(d, t)}
        src = ask.at[dom_at(d, t)]
        wants[d, t] = [
            remote(src, got_sm.at[d, t], want_sm_send.at[d, t], want_sm_recv.at[d, t], where),
            remote(src, got.at[d, t], want_send.at[d, t], want_recv.at[d, t], where),
        ]
    own_sm = local(13, ask.at[me], got_sm.at[0, 0])
    got[0, 0] = ask[me]
    for copy in early_copies:
        copy.wait()
    buddy = {"dom": dom_at(0, 1)}
    early = []
    for d in range(1, nf):
        where = {"feat": feat_at(d)}
        for i, ref in enumerate((b1_all.at[mf], b2_all.at[mf], w2_all.at[odd, mf])):
            early.append(remote(ref, ref, early_send.at[d, i], early_recv.at[d, i], where))
    hops = [
        remote(one_hbm, one_ref.at[1], pair_send.at[0], pair_recv.at[0], buddy),
        remote(two_hbm, two_ref.at[1], pair_send.at[1], pair_recv.at[1], buddy),
    ]

    feat_copy.wait()
    tiles = table_rows // LANES
    step = min(8, tiles)

    def turn(i, carry):
        for u in range(step):
            t = i * step + u
            stack = jnp.concatenate(
                [
                    feat_vm[
                        :, pl.ds(pl.multiple_of(p * table_rows + t * LANES, LANES), LANES)
                    ].astype(F32)
                    for p in range(pieces)
                ],
                axis=0,
            )
            table[pl.ds(pl.multiple_of(t * LANES, LANES), LANES), :] = jnp.transpose(stack)
        return carry

    lax.fori_loop(0, tiles // step, turn, 0)

    def gather(slot, read, wanted):
        burst = 32

        def body(i, carry):
            for u in range(burst):
                k = i * burst + u
                row = read(k) & (table_rows - 1)
                rows_vm[slot, pl.ds(k, 1), :] = table[pl.ds(row, 1), :]
            return carry

        lax.fori_loop(0, LANES // burst, body, 0)
        turned = jnp.transpose(rows_vm[slot])
        piece = wanted >> (table_rows.bit_length() - 1)
        block = jnp.zeros((height, LANES), F32)
        for p in range(pieces):
            block = jnp.where(piece == p, turned[p * height : (p + 1) * height], block)
        return block.astype(BF16)

    for copy in seed_local:
        copy.wait()
    for g in range(groups):
        seed_own[g] = gather(
            nd + g,
            lambda k: seed_sm[0, g * LANES + k],
            seed_vm[:, g * LANES : (g + 1) * LANES],
        )
    own_feat = jnp.logical_not(home)
    seed_copies = []
    for t in range(2):
        for i in range(half):
            to = odd * half + lax.rem(mf + i, half)
            which = other(t) * half + lax.rem(mf + i, half)
            copy = pltpu.make_async_remote_copy(
                src_ref=seed_own.at[which * sub // LANES],
                dst_ref=seed_all.at[mf],
                send_sem=seed_send.at[t, i],
                recv_sem=seed_recv.at[mf],
                device_id={"dom": dom_at(0, t), "feat": to},
                device_id_type=MESH,
            )
            seed_copies.append(copy)

    pl.semaphore_wait(ready, nd - 1)
    for n, copy in enumerate(seed_copies):
        if n == 0:
            pl.when(own_feat)(copy.start)
        else:
            copy.start()

    @pl.when(home)
    def _():
        seed_all[mf] = seed_own[worker * sub // LANES]

    data = {}
    for d in range(pairs):
        for t in range(2):
            if d or t:
                for copy in wants[d, t]:
                    copy.wait_recv()
            else:
                own_sm.wait()
            served[d, t] = gather(2 * d + t, lambda k: got_sm[d, t, 0, k], got[d, t])
            for e in range(half if d else 0):
                data[d, t, e] = remote(
                    served.at[d, t],
                    everyone.at[0, d, mf],
                    data_send.at[d, t * half + e],
                    data_recv.at[d, mf],
                    {"dom": dom_at(d, 0), "feat": other(t) * half + e},
                )
        if d == 0:
            for e in range(1, nf):
                to = feat_at(e)
                data[0, 0, e] = remote(
                    served.at[0, lax.rem(to // half + odd, 2)],
                    everyone.at[0, 0, mf],
                    data_send.at[0, e],
                    data_recv.at[0, mf],
                    {"feat": to},
                )
            everyone[0, 0, mf] = served[0, lax.rem(late + odd, 2)]

    def arrived(d):
        for f in range(nf):
            for_me = pltpu.make_async_copy(
                everyone.at[0, d, f], everyone.at[0, d, f], data_recv.at[d, f]
            )
            if d:
                for_me.wait()
            else:
                pl.when(mf != f)(for_me.wait)

    base = pl.multiple_of(worker * sub // LANES * LANES, LANES)
    within = lax.rem(worker * sub, LANES)
    for copy in hop_copies:
        copy.wait()
    for copy in hops:
        copy.wait_recv()
    mine = lax.rem(odd + late, 2)
    for k in range(fan2 + 1):
        if k < fan2:
            rows = two_ref[mine, k, :, pl.ds(base, LANES)]
        else:
            rows = one_ref[mine, :, pl.ds(base, LANES)]
        owner = rows >> 7
        rel = ((owner >> 1) ^ (me // 2)) + ((owner & 1) ^ odd) * pairs
        rows = (rows & (LANES - 1)) + rel * LANES
        turned = [
            pltpu.roll(rows, lax.rem(q * sub - within + LANES, LANES), 1) for q in range(per)
        ]
        for c in range(chunks):
            row = jnp.full((1, LANES), -1, jnp.int32)
            for q in range(per):
                j = c * per + q
                if j < fan1:
                    inside = (lane >= q * sub) & (lane < (q + 1) * sub)
                    row = jnp.where(inside, turned[q][j : j + 1], row)
            hop_rows[c, k : k + 1, :] = row

    slot = lax.broadcasted_iota(jnp.int32, (LANES, LANES), 0)
    each = 8
    for c in range(chunks):
        columns = slice(c * LANES, (c + 1) * LANES)
        for g in range(words.shape[0]):
            count = jnp.zeros((LANES, LANES), jnp.int32)
            for k in range(fan2):
                row = hop_rows[c, k : k + 1, :]
                rel = (row >> 7) - g * each
                real = (row >= 0) & (rel >= 0) & (rel < each)
                unit = jnp.where(real, jnp.left_shift(1, (rel & (each - 1)) * 4), 0)
                count = count + jnp.where((row & (LANES - 1)) == slot, unit, 0)
            words[g, :, columns] = count

    def build(o, carry):
        start = pl.multiple_of(o * LANES, LANES)
        place = slot + o * LANES
        shift = lax.rem(o, each) * 4
        for c in range(chunks):
            columns = slice(c * LANES, (c + 1) * LANES)
            count = lax.shift_right_logical(words[o // each, :, columns], shift) & 15
            pick_two[pl.ds(start, LANES), columns] = count.astype(F32).astype(BF16)
            pick_one[pl.ds(start, LANES), columns] = jnp.where(
                hop_rows[c, fan2 : fan2 + 1, :] == place, 1.0, 0.0
            ).astype(BF16)
        return carry

    lax.fori_loop(0, nd, build, 0)

    for copy in early:
        copy.wait_recv()
    swaps = []
    for d in range(1, nf):
        ref = w2_all.at[odd, feat_at(d)]
        swaps.append(remote(ref, ref, pair_send.at[1 + d], pair_recv.at[1 + d], buddy))
    forwards = []

    def forward(d):
        arrived(d)
        forwards.append(
            remote(everyone.at[0, d], everyone.at[1, d], pass_send.at[d], pass_recv.at[d], buddy)
        )

    for d in range(pairs):
        forward(d)
    for copy in weight_copies:
        copy.wait()
    for copy in swaps:
        copy.wait_recv()
    w2_full[...] = jnp.transpose(w2_all[...].reshape(2 * hid, w2_all.shape[3]))

    def column(rows):
        return jnp.concatenate(
            [jnp.transpose(jnp.broadcast_to(rows[f], (LANES, hid_dev))) for f in range(nf)], axis=0
        )

    b1 = column(b1_all)
    b2 = column(b2_all)
    for f in range(nf):
        for_me = pltpu.make_async_copy(seed_all.at[f], seed_all.at[f], seed_recv.at[f])
        pl.when(jnp.logical_not(home & (mf == f)))(for_me.wait)

    def whole(blocks):
        if height % 16:
            return blocks.astype(F32).reshape(depth, LANES).astype(BF16)
        return blocks.reshape(depth, LANES)

    x_seed = whole(seed_all[...]).astype(F32)
    x_seed = pltpu.roll(x_seed, lax.rem(2 * LANES - sub - within, LANES), 1)

    wide = 2 * LANES
    total = jnp.zeros((depth, LANES), F32)
    done = 0
    order = [(t, d) for t in range(2) for d in range(pairs)]
    parts = [order[:pairs], order[pairs:]]
    for i, part in enumerate(parts):
        if i:
            for copy in forwards:
                copy.wait_recv()
        fetched = jnp.concatenate([whole(everyone[t, d]) for t, d in part], axis=1)
        these = slice(done, done + len(part) * LANES)
        done += len(part) * LANES
        for n in range(chunks * LANES // wide):
            columns = slice(n * wide, (n + 1) * wide)
            own = jnp.dot(fetched, pick_one[these, columns], preferred_element_type=F32)
            mean = jnp.dot(fetched, pick_two[these, columns], preferred_element_type=F32)
            if i:
                own = own + own_sum[:, columns]
                mean = mean + mean_sum[:, columns]
            if i < len(parts) - 1:
                own_sum[:, columns] = own
                mean_sum[:, columns] = mean
                continue
            total = total + own[:, :LANES] + own[:, LANES:]
            x_all[:, columns] = own.astype(BF16)
            m_all[:, columns] = (mean * (1.0 / fan2)).astype(BF16)

    def fold(value):
        width = sub
        while width < LANES:
            value = value + pltpu.roll(value, width, 1)
            width *= 2
        return value

    is_seed = lane >= LANES - sub
    last = slice((chunks - 1) * LANES, chunks * LANES)
    m_one = fold(total) * (1.0 / fan1)
    x_all[:, last] = jnp.where(is_seed, x_seed, x_all[:, last].astype(F32)).astype(BF16)
    m_all[:, last] = jnp.where(is_seed, m_one, m_all[:, last].astype(F32)).astype(BF16)

    total = jnp.zeros((hid, LANES), F32)
    for n in range(chunks * LANES // wide):
        columns = slice(n * wide, (n + 1) * wide)
        pre = jnp.dot(w1s_ref[...], x_all[:, columns], preferred_element_type=F32)
        pre = pre + jnp.dot(w1n_ref[...], m_all[:, columns], preferred_element_type=F32)
        left = jnp.maximum(pre[:, :LANES] + b1, 0.0)
        right = jnp.maximum(pre[:, LANES:] + b1, 0.0)
        if n == chunks * LANES // wide - 1:
            h_seed = right
            right = jnp.where(is_seed, 0.0, right)
        total = total + left + right
    g_mean = fold(total) * (1.0 / fan1)
    stacked = jnp.concatenate([h_seed, g_mean], axis=0)
    z = jnp.zeros((hid, LANES), F32)
    for term in reversed(split_three(stacked)):
        z = z + jnp.dot(w2_full[...], term, preferred_element_type=F32)
    z = z + b2
    square = jnp.sum(z * z, axis=0, keepdims=True)
    z = z * lax.rsqrt(square * (1.0 / hid) + 1.0)
    part_rows = hid_dev // per
    for f in range(nf):
        packed = jnp.zeros((part_rows, LANES), F32)
        for p in range(per):
            row = f * hid_dev + p * part_rows
            value = z[row : row + part_rows]
            shift = (p * sub + sub) % LANES
            if shift:
                value = pltpu.roll(value, shift, 1)
            packed = jnp.where((lane >= p * sub) & (lane < (p + 1) * sub), value, packed)
        z_own[f] = packed

    z_copies = []
    for e in range(nf):
        to = feat_at(e)
        copy = pltpu.make_async_remote_copy(
            src_ref=z_own.at[to],
            dst_ref=z_all.at[worker],
            send_sem=z_send.at[e],
            recv_sem=z_recv.at[worker],
            device_id={"dom": 2 * (me // 2) + late, "feat": to},
            device_id_type=MESH,
        )
        z_copies.append(copy)
        if e:
            copy.start()
        else:
            pl.when(own_feat)(copy.start)

    @pl.when(home)
    def _():
        z_all[worker] = z_own[mf]

    pl.when(own_feat)(seed_copies[0].wait_send)
    sent = early + hops + swaps + forwards + seed_copies[1:] + list(data.values())
    for copy in sent + [copy for both in wants.values() for copy in both]:
        copy.wait_send()
    for w in range(nf):
        for_me = pltpu.make_async_copy(z_all.at[w], z_all.at[w], z_recv.at[w])
        pl.when(jnp.logical_not(home & (worker == w)))(for_me.wait)
    for g in range(groups):
        for p in range(per):
            block = jnp.zeros((part_rows, LANES), F32)
            for q in range(per):
                value = z_all[g * per + q]
                shift = (q - p) * sub % LANES
                if shift:
                    value = pltpu.roll(value, shift, 1)
                inside = (lane >= q * sub) & (lane < (q + 1) * sub)
                block = jnp.where(inside, value, block)
            out_ref[p * part_rows : (p + 1) * part_rows, g * LANES : (g + 1) * LANES] = block
    pl.when(own_feat)(z_copies[0].wait_send)
    for copy in z_copies[1:]:
        copy.wait_send()


def per_device(
    nd,
    nf,
    features,
    seed_rows,
    want_rows,
    live_counts,
    hop_one,
    hop_two,
    w1_self,
    w1_neigh,
    b1,
    w2_self,
    w2_neigh,
    b2,
):
    height, nodes = features.shape
    seeds = seed_rows.shape[0]
    hid_dev = b1.shape[0]
    hid, depth = w1_self.shape
    cap = want_rows.shape[2]
    fan1 = hop_one.shape[0]
    columns = (fan1 + 1) * (seeds // nf)
    groups = seeds // LANES
    vmem = pl.BlockSpec(memory_space=pltpu.VMEM)
    dma = pltpu.SemaphoreType.DMA
    return pl.pallas_call(
        functools.partial(kernel, nd, nf),
        out_shape=pltpu.VMEM((hid_dev, seeds), F32),
        in_specs=[pl.BlockSpec(memory_space=pl.ANY)] * 12,
        out_specs=vmem,
        scratch_shapes=[
            pltpu.VMEM((height, nodes), BF16),
            pltpu.VMEM((1, seeds), jnp.int32),
            pltpu.SMEM((1, seeds), jnp.int32),
            pltpu.VMEM((nd, cap), jnp.int32),
            pltpu.SMEM((1, nd), jnp.int32),
            pltpu.VMEM((2,) + hop_one.shape, jnp.int32),
            pltpu.VMEM((2,) + hop_two.shape, jnp.int32),
            pltpu.VMEM(w1_self.shape, BF16),
            pltpu.VMEM(w1_neigh.shape, BF16),
            pltpu.VMEM((nd, 1, cap), jnp.int32),
            pltpu.VMEM((nd // 2, 2, 1, cap), jnp.int32),
            pltpu.SMEM((nd // 2, 2, 1, cap), jnp.int32),
            pltpu.VMEM((nodes * height // depth, LANES), F32),
            pltpu.VMEM((nd + groups, LANES, LANES), F32),
            pltpu.VMEM((nd // 2, 2, height, cap), BF16),
            pltpu.VMEM((2, nd // 2, nf, height, cap), BF16),
            pltpu.VMEM((groups, height, LANES), BF16),
            pltpu.VMEM((nf, height, LANES), BF16),
            pltpu.VMEM((2, nf, hid_dev, w2_self.shape[0]), BF16),
            pltpu.VMEM((nf, 1, hid_dev), F32),
            pltpu.VMEM((nf, 1, hid_dev), F32),
            pltpu.VMEM((columns // LANES, 16, LANES), jnp.int32),
            pltpu.VMEM((pl.cdiv(nd, 8), LANES, columns), jnp.int32),
            pltpu.VMEM((nd * cap, columns), BF16),
            pltpu.VMEM((nd * cap, columns), BF16),
            pltpu.VMEM((depth, columns), F32),
            pltpu.VMEM((depth, columns), F32),
            pltpu.VMEM((depth, columns), BF16),
            pltpu.VMEM((depth, columns), BF16),
            pltpu.VMEM((hid, 2 * hid), BF16),
            pltpu.VMEM((nf, hid_dev * (seeds // nf) // LANES, LANES), F32),
            pltpu.VMEM((nf, hid_dev * (seeds // nf) // LANES, LANES), F32),
            dma((14,)),
            pltpu.SemaphoreType.REGULAR,
        ]
        + [dma((nd // 2, 2))] * 4
        + [dma((nd // 2, nf))] * 2
        + [dma((2, nf // 2)), dma((nf,))]
        + [dma((nf, 3))] * 2
        + [dma((nf + 1,))] * 2
        + [dma((nd // 2,))] * 2
        + [dma((nf,))] * 2,
        compiler_params=pltpu.CompilerParams(collective_id=0, has_side_effects=True),
    )(
        features,
        seed_rows.reshape(1, seeds),
        want_rows,
        live_counts,
        hop_one,
        hop_two,
        w1_self,
        w1_neigh,
        w2_self.T,
        w2_neigh.T,
        b1.reshape(1, hid_dev),
        b2.reshape(1, hid_dev),
    )


def solution(mesh):
    return jax.shard_map(
        functools.partial(per_device, mesh.shape["dom"], mesh.shape["feat"]),
        mesh=mesh,
        in_specs=(
            P("feat", "dom"),
            P("dom"),
            P("dom", None, None),
            P("dom", None),
            P(None, "dom"),
            P(None, None, "dom"),
            P(),
            P(),
            P("feat"),
            P(None, "feat"),
            P(None, "feat"),
            P("feat"),
        ),
        out_specs=P("feat", "dom"),
        check_vma=False,
    )
```

```python
import functools

import jax
import jax.numpy as jnp
from jax import lax
from jax.experimental import pallas as pl
from jax.experimental.pallas import tpu as pltpu
from jax.sharding import PartitionSpec as P

LANES = 128
MESH = pl.DeviceIdType.MESH
BF16 = jnp.bfloat16
F32 = jnp.float32


def split_three(x):
    a = x.astype(BF16)
    rest = x - a.astype(F32)
    b = rest.astype(BF16)
    c = (rest - b.astype(F32)).astype(BF16)
    return a, b, c


def kernel(
    nd,
    nf,
    feat_hbm,
    seed_hbm,
    want_hbm,
    live_hbm,
    one_hbm,
    two_hbm,
    w1s_hbm,
    w1n_hbm,
    w2s_hbm,
    w2n_hbm,
    b1_hbm,
    b2_hbm,
    out_ref,
    feat_vm,
    seed_vm,
    seed_sm,
    want_vm,
    live_sm,
    one_ref,
    two_ref,
    w1_ref,
    ask,
    ask_row,
    got,
    got_sm,
    table,
    rows_vm,
    served,
    everyone,
    seed_own,
    seed_all,
    w2_all,
    b1_all,
    b2_all,
    hop_rows,
    words,
    pick_one,
    pick_two,
    own_sum,
    mean_sum,
    xm_all,
    w2_full,
    z_own,
    z_all,
    local_sem,
    ready,
    want_send,
    want_recv,
    want_sm_send,
    want_sm_recv,
    data_send,
    data_recv,
    seed_send,
    seed_recv,
    early_send,
    early_recv,
    pair_send,
    pair_recv,
    z_send,
    z_recv,
):
    height, nodes = feat_vm.shape
    fan1, seeds = one_ref.shape
    fan2 = two_ref.shape[0]
    workers = nf // 2
    first = nf // 4
    sub = seeds // workers
    per = LANES // sub
    chunks = (fan1 + 1) * sub // LANES
    hid_dev = out_ref.shape[0]
    hid = w1_ref.shape[0]
    depth = w1_ref.shape[1] // 2
    part_rows = hid_dev // per
    groups = seeds // LANES
    pieces = depth // height
    table_rows = nodes // pieces
    me = lax.axis_index("dom")
    mf = lax.axis_index("feat")
    pairs = nd // 2
    odd = lax.rem(me, 2)
    mine = mf - first
    works = (mf >= first) & (mf < first + workers)

    def flip(x, bits):
        bit = 1
        while bit <= bits:
            if bits & bit:
                x = x + bit * (1 - 2 * lax.rem(x // bit, 2))
            bit *= 2
        return x

    def other(t):
        return odd + t * (1 - 2 * odd)

    def dom_at(d, t):
        return 2 * flip(me // 2, d) + other(t)

    def feat_at(d):
        return lax.rem(mf + d, nf)

    def local(i, src, dst):
        copy = pltpu.make_async_copy(src, dst, local_sem.at[i])
        copy.start()
        return copy

    barrier = pltpu.get_barrier_semaphore()
    for d in range(1, nf):
        pl.semaphore_signal(barrier, inc=1, device_id={"feat": feat_at(d)}, device_id_type=MESH)
    peers = [(d, t) for d in range(pairs) for t in range(2)][1:]
    for d, t in peers:
        pl.semaphore_signal(barrier, inc=1, device_id={"dom": dom_at(d, t)}, device_id_type=MESH)

    want_copies = [local(0, want_hbm.at[0], want_vm), local(1, live_hbm, live_sm)]
    feat_copy = local(2, feat_hbm, feat_vm)
    early_copies = [
        local(3, w2s_hbm, w2_all.at[0, mf]),
        local(4, w2n_hbm, w2_all.at[1, mf]),
        local(5, b1_hbm, b1_all.at[mf]),
        local(6, b2_hbm, b2_all.at[mf]),
    ]
    seed_local = [local(7, seed_hbm, seed_vm), local(8, seed_hbm, seed_sm)]
    hop_copies = [
        pltpu.make_async_copy(one_hbm, one_ref, local_sem.at[9]),
        pltpu.make_async_copy(two_hbm, two_ref, local_sem.at[10]),
    ]
    weight_copies = [
        pltpu.make_async_copy(w1s_hbm, w1_ref.at[:, :depth], local_sem.at[11]),
        pltpu.make_async_copy(w1n_hbm, w1_ref.at[:, depth:], local_sem.at[12]),
    ]

    @pl.when(works)
    def _():
        for copy in hop_copies + weight_copies:
            copy.start()

    def remote(src, dst, send, recv, where):
        copy = pltpu.make_async_remote_copy(
            src_ref=src,
            dst_ref=dst,
            send_sem=send,
            recv_sem=recv,
            device_id=where,
            device_id_type=MESH,
        )
        copy.start()
        return copy

    lane = lax.broadcasted_iota(jnp.int32, (1, LANES), 1)
    for copy in want_copies:
        copy.wait()
    for o in range(nd):
        wanted = jnp.where(lane < live_sm[0, o], want_vm[o : o + 1], -1)
        ask[o] = wanted
        ask_row[o] = wanted & (table_rows - 1)
    pl.semaphore_wait(barrier, nd + nf - 2)

    for d, t in peers:
        pl.semaphore_signal(ready, inc=1, device_id={"dom": dom_at(d, t)}, device_id_type=MESH)
    wants = {}
    for d, t in peers:
        where = {"dom": dom_at(d, t)}
        to = dom_at(d, t)
        sem = want_sm_send.at[d, t], want_sm_recv.at[d, t]
        wants[d, t] = [
            remote(ask_row.at[to], got_sm.at[d, t], *sem, where),
            remote(ask.at[to], got.at[d, t], want_send.at[d, t], want_recv.at[d, t], where),
        ]
    own_sm = local(13, ask_row.at[me], got_sm.at[0, 0])
    got[0, 0] = ask[me]
    for copy in early_copies:
        copy.wait()
    buddy = {"dom": dom_at(0, 1)}

    def to_worker(w, src, dst, send, recv, where):
        copy = pltpu.make_async_remote_copy(
            src_ref=src,
            dst_ref=dst,
            send_sem=send,
            recv_sem=recv,
            device_id={**where, "feat": first + w},
            device_id_type=MESH,
        )
        pl.when(mf != first + w)(copy.start)
        loose.append((w, copy))

    def landed(ref, sem, f):
        copy = pltpu.make_async_copy(ref, ref, sem)
        pl.when(mf != f)(copy.wait)

    loose = []
    for w in range(workers):
        for i, ref in enumerate((b1_all.at[mf], b2_all.at[mf], w2_all.at[odd, mf])):
            to_worker(w, ref, ref, early_send.at[w, i], early_recv.at[mf, i], {})

    feat_copy.wait()
    tiles = table_rows // LANES
    step = min(8, tiles)

    def turn(i, carry):
        for u in range(step):
            t = i * step + u
            stack = jnp.concatenate(
                [
                    feat_vm[
                        :, pl.ds(pl.multiple_of(p * table_rows + t * LANES, LANES), LANES)
                    ].astype(F32)
                    for p in range(pieces)
                ],
                axis=0,
            )
            table[pl.ds(pl.multiple_of(t * LANES, LANES), LANES), :] = jnp.transpose(stack)
        return carry

    lax.fori_loop(0, tiles // step, turn, 0)

    def gather(jobs):
        for slot, read, _ in jobs:
            for k in range(LANES):
                rows_vm[slot, k : k + 1, :] = table[pl.ds(read(k), 1), :]
        blocks = []
        for slot, _, wanted in jobs:
            turned = jnp.transpose(rows_vm[slot])
            piece = wanted >> (table_rows.bit_length() - 1)
            block = jnp.zeros((height, LANES), F32)
            for p in range(pieces):
                block = jnp.where(piece == p, turned[p * height : (p + 1) * height], block)
            blocks.append(block.astype(BF16))
        return blocks

    for copy in seed_local:
        copy.wait()
    def seed_job(g):
        at = g * LANES
        return (
            nd + g,
            lambda k: seed_sm[0, at + k] & (table_rows - 1),
            seed_vm[:, at : at + LANES],
        )

    for g, block in enumerate(gather([seed_job(g) for g in range(groups)])):
        seed_own[g] = block
    for w in range(workers):
        block = seed_own.at[w * sub // LANES]
        to_worker(w, block, seed_all.at[mf], seed_send.at[w], seed_recv.at[mf], {})

    @pl.when(works)
    def _():
        seed_all[mf] = seed_own[mine * sub // LANES]

    pl.semaphore_wait(ready, nd - 1)
    base = pl.multiple_of(mine * sub // LANES * LANES, LANES)
    within = lax.rem(mine * sub, LANES)
    slot = lax.broadcasted_iota(jnp.int32, (LANES, LANES), 0)
    each = 8
    picked = chunks if per > 1 else chunks - 1

    def prepare():
        for copy in hop_copies:
            copy.wait()
        for k in range(fan2 + 1):
            if k < fan2:
                rows = two_ref[k, :, pl.ds(base, LANES)]
            else:
                rows = one_ref[:, pl.ds(base, LANES)]
            owner = rows >> 7
            rel = ((owner >> 1) ^ (me // 2)) * 2 + ((owner & 1) ^ odd)
            rows = (rows & (LANES - 1)) + rel * LANES
            turned = [
                pltpu.roll(rows, lax.rem(q * sub - within + LANES, LANES), 1) for q in range(per)
            ]
            for c in range(chunks):
                row = jnp.full((1, LANES), -1, jnp.int32)
                for q in range(per):
                    j = c * per + q
                    if j < fan1:
                        inside = (lane >= q * sub) & (lane < (q + 1) * sub)
                        row = jnp.where(inside, turned[q][j : j + 1], row)
                hop_rows[c, k : k + 1, :] = row

        for c in range(picked):
            columns = slice(c * LANES, (c + 1) * LANES)
            for g in range(words.shape[0]):
                count = jnp.zeros((LANES, LANES), jnp.int32)
                for k in range(fan2):
                    row = hop_rows[c, k : k + 1, :]
                    rel = (row >> 7) - g * each
                    real = (row >= 0) & (rel >= 0) & (rel < each)
                    unit = jnp.where(real, jnp.left_shift(1, (rel & (each - 1)) * 4), 0)
                    count = count + jnp.where((row & (LANES - 1)) == slot, unit, 0)
                words[g, :, columns] = count

    @pl.when(works)
    def _():
        prepare()

    def work():
        def expand(owners):
            for o in owners:
                place = slot + o * LANES
                these = slice(o * LANES, (o + 1) * LANES)
                for c in range(picked):
                    columns = slice(c * LANES, (c + 1) * LANES)
                    count = lax.shift_right_logical(words[o // each, :, columns], o % each * 4)
                    pick_two[these, columns] = (count & 15).astype(F32).astype(BF16)
                    pick_one[these, columns] = jnp.where(
                        hop_rows[c, fan2 : fan2 + 1, :] == place, 1.0, 0.0
                    ).astype(BF16)

        steps = min(4, pairs)
        ends = [nd * i // steps for i in range(steps + 1)]
        expand(range(ends[0], ends[1]))
        for f in range(nf):
            for i, ref in enumerate((b1_all.at[f], b2_all.at[f], w2_all.at[odd, f])):
                landed(ref, early_recv.at[f, i], f)
        swaps = []
        for d in range(1, nf):
            ref = w2_all.at[odd, feat_at(d)]
            swaps.append(remote(ref, ref, pair_send.at[d], pair_recv.at[d], buddy))
        for copy in weight_copies:
            copy.wait()
        for copy in swaps:
            copy.wait_recv()
        w2_full[...] = jnp.transpose(w2_all[...].reshape(2 * hid, w2_all.shape[3]))

        def column(rows):
            return jnp.concatenate(
                [jnp.transpose(jnp.broadcast_to(rows[f], (LANES, hid_dev))) for f in range(nf)], axis=0
            )

        b1 = column(b1_all)
        b2 = column(b2_all)
        for f in range(nf):
            landed(seed_all.at[f], seed_recv.at[f], f)

        def whole(blocks):
            if height % 16:
                return blocks.astype(F32).reshape(depth, LANES).astype(BF16)
            return blocks.reshape(depth, LANES)

        x_seed = whole(seed_all[...]).astype(F32)
        if per > 1:
            x_seed = pltpu.roll(x_seed, lax.rem(2 * LANES - sub - within, LANES), 1)

        wide = 2 * LANES
        total = jnp.zeros((depth, LANES), F32)
        done = 0
        for i in range(steps):
            part = [(o // 2, o % 2) for o in range(ends[i], ends[i + 1])]
            if i + 1 < steps:
                expand(range(ends[i + 1], ends[i + 2]))
            for d, t in part:
                for f in range(nf):
                    if d or t:
                        spot = everyone.at[d, t, f]
                        pltpu.make_async_copy(spot, spot, data_recv.at[d, t, f]).wait()
                    else:
                        landed(everyone.at[0, 0, f], data_recv.at[0, 0, f], f)
            fetched = jnp.concatenate([whole(everyone[d, t]) for d, t in part], axis=1)
            these = slice(done, done + len(part) * LANES)
            done += len(part) * LANES
            for n in range(0, picked, 2):
                columns = slice(n * LANES, min(n + 2, picked) * LANES)
                own = jnp.dot(fetched, pick_one[these, columns], preferred_element_type=F32)
                mean = jnp.dot(fetched, pick_two[these, columns], preferred_element_type=F32)
                if i:
                    own = own + own_sum[:, columns]
                    mean = mean + mean_sum[:, columns]
                if i < steps - 1:
                    own_sum[:, columns] = own
                    mean_sum[:, columns] = mean
                    continue
                for at in range(0, own.shape[1], LANES):
                    total = total + own[:, at : at + LANES]
                xm_all[:depth, columns] = own.astype(BF16)
                xm_all[depth:, columns] = (mean * (1.0 / fan2)).astype(BF16)

        def fold(value):
            width = sub
            while width < LANES:
                value = value + pltpu.roll(value, width, 1)
                width *= 2
            return value

        is_seed = lane >= LANES - sub
        last = slice((chunks - 1) * LANES, chunks * LANES)
        m_one = fold(total) * (1.0 / fan1)
        if per > 1:
            x_seed = jnp.where(is_seed, x_seed, xm_all[:depth, last].astype(F32))
            m_one = jnp.where(is_seed, m_one, xm_all[depth:, last].astype(F32))
        xm_all[:depth, last] = x_seed.astype(BF16)
        xm_all[depth:, last] = m_one.astype(BF16)

        total = jnp.zeros((hid, LANES), F32)
        for n in range(chunks * LANES // wide):
            columns = slice(n * wide, (n + 1) * wide)
            pre = jnp.dot(w1_ref[...], xm_all[:, columns], preferred_element_type=F32)
            left = jnp.maximum(pre[:, :LANES] + b1, 0.0)
            right = jnp.maximum(pre[:, LANES:] + b1, 0.0)
            if n == chunks * LANES // wide - 1:
                h_seed = right
                right = jnp.where(is_seed, 0.0, right)
            total = total + left + right
        g_mean = fold(total) * (1.0 / fan1)
        stacked = jnp.concatenate([h_seed, g_mean], axis=0)
        z = jnp.zeros((hid, LANES), F32)
        for term in reversed(split_three(stacked)):
            z = z + jnp.dot(w2_full[...], term, preferred_element_type=F32)
        z = z + b2
        square = jnp.sum(z * z, axis=0, keepdims=True)
        z = z * lax.rsqrt(square * (1.0 / hid) + 1.0)
        for f in range(nf):
            packed = jnp.zeros((part_rows, LANES), F32)
            for p in range(per):
                row = f * hid_dev + p * part_rows
                value = z[row : row + part_rows]
                shift = (p * sub + sub) % LANES
                if shift:
                    value = pltpu.roll(value, shift, 1)
                packed = jnp.where((lane >= p * sub) & (lane < (p + 1) * sub), value, packed)
            z_own[f] = packed

        z_copies = []
        for e in range(1, nf):
            to = feat_at(e)
            where = {"feat": to}
            z_copies.append(remote(z_own.at[to], z_all.at[mine], z_send.at[e], z_recv.at[mine], where))
        z_all[mine] = z_own[mf]
        for copy in swaps + z_copies:
            copy.wait_send()

    data = []
    def want_job(d, t):
        return (2 * d + t, lambda k: got_sm[d, t, 0, k], got[d, t])

    for d in range(pairs):
        for t in range(2):
            if d or t:
                for copy in wants[d, t]:
                    copy.wait_recv()
            else:
                own_sm.wait()
        for t, block in enumerate(gather([want_job(d, t) for t in range(2)])):
            served[d, t] = block
            for w in range(workers):
                block = served.at[d, t]
                spot = everyone.at[d, t, mf]
                send = data_send.at[d, t, w]
                recv = data_recv.at[d, t, mf]
                if d or t:
                    where = {"dom": dom_at(d, t), "feat": first + w}
                    data.append(remote(block, spot, send, recv, where))
                else:
                    to_worker(w, block, spot, send, recv, {})
    everyone[0, 0, mf] = served[0, 0]

    @pl.when(works)
    def _():
        work()

    for w, copy in loose:
        pl.when(mf != first + w)(copy.wait_send)
    for copy in data + [copy for both in wants.values() for copy in both]:
        copy.wait_send()
    for w in range(workers):
        landed(z_all.at[w], z_recv.at[w], first + w)
    for g in range(groups):
        for p in range(per):
            block = jnp.zeros((part_rows, LANES), F32)
            for q in range(per):
                value = z_all[g * per + q]
                shift = (q - p) * sub % LANES
                if shift:
                    value = pltpu.roll(value, shift, 1)
                inside = (lane >= q * sub) & (lane < (q + 1) * sub)
                block = jnp.where(inside, value, block)
            out_ref[p * part_rows : (p + 1) * part_rows, g * LANES : (g + 1) * LANES] = block

def per_device(
    nd,
    nf,
    features,
    seed_rows,
    want_rows,
    live_counts,
    hop_one,
    hop_two,
    w1_self,
    w1_neigh,
    b1,
    w2_self,
    w2_neigh,
    b2,
):
    height, nodes = features.shape
    seeds = seed_rows.shape[0]
    hid_dev = b1.shape[0]
    hid, depth = w1_self.shape
    cap = want_rows.shape[2]
    fan1 = hop_one.shape[0]
    workers = nf // 2
    columns = (fan1 + 1) * (seeds // workers)
    result = (hid_dev * (seeds // workers) // LANES, LANES)
    groups = seeds // LANES
    vmem = pl.BlockSpec(memory_space=pltpu.VMEM)
    dma = pltpu.SemaphoreType.DMA
    return pl.pallas_call(
        functools.partial(kernel, nd, nf),
        out_shape=pltpu.VMEM((hid_dev, seeds), F32),
        in_specs=[pl.BlockSpec(memory_space=pl.ANY)] * 12,
        out_specs=vmem,
        scratch_shapes=[
            pltpu.VMEM((height, nodes), BF16),
            pltpu.VMEM((1, seeds), jnp.int32),
            pltpu.SMEM((1, seeds), jnp.int32),
            pltpu.VMEM((nd, cap), jnp.int32),
            pltpu.SMEM((1, nd), jnp.int32),
            pltpu.VMEM(hop_one.shape, jnp.int32),
            pltpu.VMEM(hop_two.shape, jnp.int32),
            pltpu.VMEM((hid, 2 * depth), BF16),
            pltpu.VMEM((nd, 1, cap), jnp.int32),
            pltpu.VMEM((nd, 1, cap), jnp.int32),
            pltpu.VMEM((nd // 2, 2, 1, cap), jnp.int32),
            pltpu.SMEM((nd // 2, 2, 1, cap), jnp.int32),
            pltpu.VMEM((nodes * height // depth, LANES), F32),
            pltpu.VMEM((nd + groups, LANES, LANES), F32),
            pltpu.VMEM((nd // 2, 2, height, cap), BF16),
            pltpu.VMEM((nd // 2, 2, nf, height, cap), BF16),
            pltpu.VMEM((groups, height, LANES), BF16),
            pltpu.VMEM((nf, height, LANES), BF16),
            pltpu.VMEM((2, nf, hid_dev, w2_self.shape[0]), BF16),
            pltpu.VMEM((nf, 1, hid_dev), F32),
            pltpu.VMEM((nf, 1, hid_dev), F32),
            pltpu.VMEM((columns // LANES, 16, LANES), jnp.int32),
            pltpu.VMEM((pl.cdiv(nd, 8), LANES, columns), jnp.int32),
            pltpu.VMEM((nd * cap, columns), BF16),
            pltpu.VMEM((nd * cap, columns), BF16),
            pltpu.VMEM((depth, columns), F32),
            pltpu.VMEM((depth, columns), F32),
            pltpu.VMEM((2 * depth, columns), BF16),
            pltpu.VMEM((hid, 2 * hid), BF16),
            pltpu.VMEM((nf,) + result, F32),
            pltpu.VMEM((workers,) + result, F32),
            dma((14,)),
            pltpu.SemaphoreType.REGULAR,
        ]
        + [dma((nd // 2, 2))] * 4
        + [dma((nd // 2, 2, workers)), dma((nd // 2, 2, nf))]
        + [dma((workers,)), dma((nf,))]
        + [dma((workers, 3)), dma((nf, 3))]
        + [dma((nf,))] * 2
        + [dma((nf,)), dma((workers,))],
        compiler_params=pltpu.CompilerParams(collective_id=0, has_side_effects=True),
    )(
        features,
        seed_rows.reshape(1, seeds),
        want_rows,
        live_counts,
        hop_one,
        hop_two,
        w1_self,
        w1_neigh,
        w2_self.T,
        w2_neigh.T,
        b1.reshape(1, hid_dev),
        b2.reshape(1, hid_dev),
    )


def solution(mesh):
    return jax.shard_map(
        functools.partial(per_device, mesh.shape["dom"], mesh.shape["feat"]),
        mesh=mesh,
        in_specs=(
            P("feat", "dom"),
            P("dom"),
            P("dom", None, None),
            P("dom", None),
            P(None, "dom"),
            P(None, None, "dom"),
            P(),
            P(),
            P("feat"),
            P(None, "feat"),
            P(None, "feat"),
            P("feat"),
        ),
        out_specs=P("feat", "dom"),
        check_vma=False,
    )
```

```python
import functools

import jax
import jax.numpy as jnp
from jax import lax
from jax.experimental import pallas as pl
from jax.experimental.pallas import tpu as pltpu
from jax.sharding import PartitionSpec as P

LANES = 128
MESH = pl.DeviceIdType.MESH
BF16 = jnp.bfloat16
F32 = jnp.float32


def split_three(x):
    a = x.astype(BF16)
    rest = x - a.astype(F32)
    b = rest.astype(BF16)
    c = (rest - b.astype(F32)).astype(BF16)
    return a, b, c


def kernel(
    nd,
    nf,
    feat_hbm,
    seed_hbm,
    want_hbm,
    live_hbm,
    one_hbm,
    two_hbm,
    w1s_hbm,
    w1n_hbm,
    w2s_hbm,
    w2n_hbm,
    b1_hbm,
    b2_hbm,
    out_ref,
    feat_vm,
    seed_vm,
    seed_sm,
    want_vm,
    live_sm,
    one_ref,
    two_ref,
    w1_ref,
    ask,
    ask_row,
    got,
    got_sm,
    table,
    rows_vm,
    served,
    everyone,
    seed_own,
    seed_all,
    w2_all,
    b1_all,
    b2_all,
    hop_rows,
    words,
    pick_one,
    pick_two,
    own_sum,
    mean_sum,
    xm_all,
    w2_full,
    z_own,
    z_all,
    local_sem,
    ready,
    want_send,
    want_recv,
    want_sm_send,
    want_sm_recv,
    data_send,
    data_recv,
    seed_send,
    seed_recv,
    early_send,
    early_recv,
    pair_send,
    pair_recv,
    z_send,
    z_recv,
):
    height, nodes = feat_vm.shape
    fan1, seeds = one_ref.shape
    fan2 = two_ref.shape[0]
    workers = nf // 2
    first = nf // 4
    sub = seeds // workers
    per = LANES // sub
    chunks = (fan1 + 1) * sub // LANES
    hid_dev = out_ref.shape[0]
    hid = w1_ref.shape[0]
    depth = w1_ref.shape[1] // 2
    part_rows = hid_dev // per
    groups = seeds // LANES
    pieces = depth // height
    table_rows = nodes // pieces
    me = lax.axis_index("dom")
    mf = lax.axis_index("feat")
    pairs = nd // 2
    odd = lax.rem(me, 2)
    mine = mf - first
    works = (mf >= first) & (mf < first + workers)

    def flip(x, bits):
        bit = 1
        while bit <= bits:
            if bits & bit:
                x = x + bit * (1 - 2 * lax.rem(x // bit, 2))
            bit *= 2
        return x

    def other(t):
        return odd + t * (1 - 2 * odd)

    def dom_at(d, t):
        return 2 * flip(me // 2, d) + other(t)

    def feat_at(d):
        return lax.rem(mf + d, nf)

    def local(i, src, dst):
        copy = pltpu.make_async_copy(src, dst, local_sem.at[i])
        copy.start()
        return copy

    barrier = pltpu.get_barrier_semaphore()
    for d in range(1, nf):
        pl.semaphore_signal(barrier, inc=1, device_id={"feat": feat_at(d)}, device_id_type=MESH)
    peers = [(d, t) for d in range(pairs) for t in range(2)][1:]
    for d, t in peers:
        pl.semaphore_signal(barrier, inc=1, device_id={"dom": dom_at(d, t)}, device_id_type=MESH)

    want_copies = [local(0, want_hbm.at[0], want_vm), local(1, live_hbm, live_sm)]
    feat_copy = local(2, feat_hbm, feat_vm)
    early_copies = [
        local(3, w2s_hbm, w2_all.at[0, mf]),
        local(4, w2n_hbm, w2_all.at[1, mf]),
        local(5, b1_hbm, b1_all.at[mf]),
        local(6, b2_hbm, b2_all.at[mf]),
    ]
    seed_local = [local(7, seed_hbm, seed_vm), local(8, seed_hbm, seed_sm)]
    hop_copies = [
        pltpu.make_async_copy(one_hbm, one_ref, local_sem.at[9]),
        pltpu.make_async_copy(two_hbm, two_ref, local_sem.at[10]),
    ]
    weight_copies = [
        pltpu.make_async_copy(w1s_hbm, w1_ref.at[:, :depth], local_sem.at[11]),
        pltpu.make_async_copy(w1n_hbm, w1_ref.at[:, depth:], local_sem.at[12]),
    ]

    @pl.when(works)
    def _():
        for copy in hop_copies + weight_copies:
            copy.start()

    def remote(src, dst, send, recv, where):
        copy = pltpu.make_async_remote_copy(
            src_ref=src,
            dst_ref=dst,
            send_sem=send,
            recv_sem=recv,
            device_id=where,
            device_id_type=MESH,
        )
        copy.start()
        return copy

    lane = lax.broadcasted_iota(jnp.int32, (1, LANES), 1)
    for copy in want_copies:
        copy.wait()
    for o in range(nd):
        wanted = jnp.where(lane < live_sm[0, o], want_vm[o : o + 1], -1)
        ask[o] = wanted
        ask_row[o] = wanted & (table_rows - 1)
    feat_copy.wait()
    tiles = table_rows // LANES
    step = min(8, tiles)

    def turn(i, carry):
        for u in range(step):
            t = i * step + u
            stack = jnp.concatenate(
                [
                    feat_vm[
                        :, pl.ds(pl.multiple_of(p * table_rows + t * LANES, LANES), LANES)
                    ].astype(F32)
                    for p in range(pieces)
                ],
                axis=0,
            )
            table[pl.ds(pl.multiple_of(t * LANES, LANES), LANES), :] = jnp.transpose(stack)
        return carry

    lax.fori_loop(0, tiles // step, turn, 0)

    base = pl.multiple_of(mine * sub // LANES * LANES, LANES)
    within = lax.rem(mine * sub, LANES)
    slot = lax.broadcasted_iota(jnp.int32, (LANES, LANES), 0)
    each = 8
    picked = chunks if per > 1 else chunks - 1

    @pl.when(works)
    def _():
        for copy in hop_copies:
            copy.wait()
        for k in range(fan2 + 1):
            if k < fan2:
                rows = two_ref[k, :, pl.ds(base, LANES)]
            else:
                rows = one_ref[:, pl.ds(base, LANES)]
            owner = rows >> 7
            rel = ((owner >> 1) ^ (me // 2)) * 2 + ((owner & 1) ^ odd)
            rows = (rows & (LANES - 1)) + rel * LANES
            turned = [
                pltpu.roll(rows, lax.rem(q * sub - within + LANES, LANES), 1) for q in range(per)
            ]
            for c in range(chunks):
                row = jnp.full((1, LANES), -1, jnp.int32)
                for q in range(per):
                    j = c * per + q
                    if j < fan1:
                        inside = (lane >= q * sub) & (lane < (q + 1) * sub)
                        row = jnp.where(inside, turned[q][j : j + 1], row)
                hop_rows[c, k : k + 1, :] = row

    pl.semaphore_wait(barrier, nd + nf - 2)

    for d, t in peers:
        pl.semaphore_signal(ready, inc=1, device_id={"dom": dom_at(d, t)}, device_id_type=MESH)
    wants = {}
    for d, t in peers:
        where = {"dom": dom_at(d, t)}
        to = dom_at(d, t)
        sem = want_sm_send.at[d, t], want_sm_recv.at[d, t]
        wants[d, t] = [
            remote(ask_row.at[to], got_sm.at[d, t], *sem, where),
            remote(ask.at[to], got.at[d, t], want_send.at[d, t], want_recv.at[d, t], where),
        ]
    own_sm = local(13, ask_row.at[me], got_sm.at[0, 0])
    got[0, 0] = ask[me]
    for copy in early_copies:
        copy.wait()
    buddy = {"dom": dom_at(0, 1)}

    def to_worker(w, src, dst, send, recv, where):
        copy = pltpu.make_async_remote_copy(
            src_ref=src,
            dst_ref=dst,
            send_sem=send,
            recv_sem=recv,
            device_id={**where, "feat": first + w},
            device_id_type=MESH,
        )
        pl.when(mf != first + w)(copy.start)
        loose.append((w, copy))

    def landed(ref, sem, f):
        copy = pltpu.make_async_copy(ref, ref, sem)
        pl.when(mf != f)(copy.wait)

    loose = []
    for w in range(workers):
        for i, ref in enumerate((b1_all.at[mf], b2_all.at[mf], w2_all.at[odd, mf])):
            to_worker(w, ref, ref, early_send.at[w, i], early_recv.at[mf, i], {})

    def gather(jobs):
        for slot, read, _ in jobs:
            for k in range(LANES):
                rows_vm[slot, k : k + 1, :] = table[pl.ds(read(k), 1), :]
        blocks = []
        for slot, _, wanted in jobs:
            turned = jnp.transpose(rows_vm[slot])
            piece = wanted >> (table_rows.bit_length() - 1)
            block = jnp.zeros((height, LANES), F32)
            for p in range(pieces):
                block = jnp.where(piece == p, turned[p * height : (p + 1) * height], block)
            blocks.append(block.astype(BF16))
        return blocks

    for copy in seed_local:
        copy.wait()
    def seed_job(g):
        at = g * LANES
        return (
            nd + g,
            lambda k: seed_sm[0, at + k] & (table_rows - 1),
            seed_vm[:, at : at + LANES],
        )

    for g, block in enumerate(gather([seed_job(g) for g in range(groups)])):
        seed_own[g] = block
    for w in range(workers):
        block = seed_own.at[w * sub // LANES]
        to_worker(w, block, seed_all.at[mf], seed_send.at[w], seed_recv.at[mf], {})

    @pl.when(works)
    def _():
        seed_all[mf] = seed_own[mine * sub // LANES]

    steps = min(4, pairs)
    ends = [nd * i // steps for i in range(steps + 1)]

    def expand(i, c):
        columns = slice(c * LANES, (c + 1) * LANES)
        short = jnp.int16
        row = jnp.broadcast_to(hop_rows[c, fan2 : fan2 + 1, :], (16, LANES)).astype(short)
        row = jnp.concatenate([row] * (LANES // 16), axis=0)
        for o in range(ends[i], ends[i + 1]):
            these = slice(o * LANES, (o + 1) * LANES)
            count = lax.shift_right_logical(words[o // each, :, columns], o % each * 4) & 15
            pick_two[these, columns] = count.astype(F32).astype(BF16)
            same = row == (slot + o * LANES).astype(short)
            pick_one[these, columns] = jnp.where(same, jnp.ones((), BF16), jnp.zeros((), BF16))

    def prepare():
        for c in range(picked):
            columns = slice(c * LANES, (c + 1) * LANES)
            for g in range(words.shape[0]):
                count = jnp.zeros((LANES, LANES), jnp.int32)
                for k in range(fan2):
                    row = hop_rows[c, k : k + 1, :]
                    rel = (row >> 7) - g * each
                    real = (row >= 0) & (rel >= 0) & (rel < each)
                    unit = jnp.where(real, jnp.left_shift(1, (rel & (each - 1)) * 4), 0)
                    count = count + jnp.where((row & (LANES - 1)) == slot, unit, 0)
                words[g, :, columns] = count

    def work():
        for f in range(nf):
            for i, ref in enumerate((b1_all.at[f], b2_all.at[f], w2_all.at[odd, f])):
                landed(ref, early_recv.at[f, i], f)
        swaps = []
        for d in range(1, nf):
            ref = w2_all.at[odd, feat_at(d)]
            swaps.append(remote(ref, ref, pair_send.at[d], pair_recv.at[d], buddy))
        def column(rows):
            return jnp.concatenate(
                [jnp.transpose(jnp.broadcast_to(rows[f], (LANES, hid_dev))) for f in range(nf)], axis=0
            )

        b1 = column(b1_all)
        b2 = column(b2_all)
        for c in range(picked if steps > 1 else 0):
            expand(1, c)
        for f in range(nf):
            landed(seed_all.at[f], seed_recv.at[f], f)

        def whole(blocks):
            if height % 16:
                return blocks.astype(F32).reshape(depth, LANES).astype(BF16)
            return blocks.reshape(depth, LANES)

        x_seed = whole(seed_all[...]).astype(F32)
        if per > 1:
            x_seed = pltpu.roll(x_seed, lax.rem(2 * LANES - sub - within, LANES), 1)

        wide = 2 * LANES
        total = jnp.zeros((depth, LANES), F32)
        done = 0
        for i in range(steps):
            part = [(o // 2, o % 2) for o in range(ends[i], ends[i + 1])]
            if i == 1:
                for later in range(2, steps):
                    for c in range(picked):
                        expand(later, c)
                for copy in weight_copies:
                    copy.wait()
                for copy in swaps:
                    copy.wait_recv()
                w2_full[...] = jnp.transpose(w2_all[...].reshape(2 * hid, w2_all.shape[3]))
            for d, t in part:
                for f in range(nf):
                    if d or t:
                        spot = everyone.at[d, t, f]
                        pltpu.make_async_copy(spot, spot, data_recv.at[d, t, f]).wait()
                    else:
                        landed(everyone.at[0, 0, f], data_recv.at[0, 0, f], f)
            fetched = jnp.concatenate([whole(everyone[d, t]) for d, t in part], axis=1)
            these = slice(done, done + len(part) * LANES)
            done += len(part) * LANES
            for n in range(0, picked, 2):
                columns = slice(n * LANES, min(n + 2, picked) * LANES)
                own = jnp.dot(fetched, pick_one[these, columns], preferred_element_type=F32)
                mean = jnp.dot(fetched, pick_two[these, columns], preferred_element_type=F32)
                if i:
                    own = own + own_sum[:, columns]
                    mean = mean + mean_sum[:, columns]
                if i < steps - 1:
                    own_sum[:, columns] = own
                    mean_sum[:, columns] = mean
                    continue
                for at in range(0, own.shape[1], LANES):
                    total = total + own[:, at : at + LANES]
                xm_all[:depth, columns] = own.astype(BF16)
                xm_all[depth:, columns] = (mean * (1.0 / fan2)).astype(BF16)

        def fold(value):
            width = sub
            while width < LANES:
                value = value + pltpu.roll(value, width, 1)
                width *= 2
            return value

        is_seed = lane >= LANES - sub
        last = slice((chunks - 1) * LANES, chunks * LANES)
        m_one = fold(total) * (1.0 / fan1)
        if per > 1:
            x_seed = jnp.where(is_seed, x_seed, xm_all[:depth, last].astype(F32))
            m_one = jnp.where(is_seed, m_one, xm_all[depth:, last].astype(F32))
        xm_all[:depth, last] = x_seed.astype(BF16)
        xm_all[depth:, last] = m_one.astype(BF16)

        total = jnp.zeros((hid, LANES), F32)
        for n in range(chunks * LANES // wide):
            columns = slice(n * wide, (n + 1) * wide)
            pre = jnp.dot(w1_ref[...], xm_all[:, columns], preferred_element_type=F32)
            left = jnp.maximum(pre[:, :LANES] + b1, 0.0)
            right = jnp.maximum(pre[:, LANES:] + b1, 0.0)
            if n == chunks * LANES // wide - 1:
                h_seed = right
                right = jnp.where(is_seed, 0.0, right)
            total = total + left + right
        g_mean = fold(total) * (1.0 / fan1)
        stacked = jnp.concatenate([h_seed, g_mean], axis=0)
        z = jnp.zeros((hid, LANES), F32)
        for term in reversed(split_three(stacked)):
            z = z + jnp.dot(w2_full[...], term, preferred_element_type=F32)
        z = z + b2
        square = jnp.sum(z * z, axis=0, keepdims=True)
        z = z * lax.rsqrt(square * (1.0 / hid) + 1.0)
        for f in range(nf):
            packed = jnp.zeros((part_rows, LANES), F32)
            for p in range(per):
                row = f * hid_dev + p * part_rows
                value = z[row : row + part_rows]
                shift = (p * sub + sub) % LANES
                if shift:
                    value = pltpu.roll(value, shift, 1)
                packed = jnp.where((lane >= p * sub) & (lane < (p + 1) * sub), value, packed)
            z_own[f] = packed

        z_copies = []
        for e in range(1, nf):
            to = feat_at(e)
            where = {"feat": to}
            z_copies.append(remote(z_own.at[to], z_all.at[mine], z_send.at[e], z_recv.at[mine], where))
        z_all[mine] = z_own[mf]
        for copy in swaps + z_copies:
            copy.wait_send()

    data = []
    def want_job(d, t):
        return (2 * d + t, lambda k: got_sm[d, t, 0, k], got[d, t])

    def serve(d):
        for t in range(2):
            if d or t:
                for copy in wants[d, t]:
                    copy.wait_recv()
            else:
                own_sm.wait()
        for t, block in enumerate(gather([want_job(d, t) for t in range(2)])):
            served[d, t] = block
            if d:
                deliver(d, t)

    def deliver(d, t):
        for w in range(workers):
            block = served.at[d, t]
            spot = everyone.at[d, t, mf]
            send = data_send.at[d, t, w]
            recv = data_recv.at[d, t, mf]
            if d or t:
                where = {"dom": dom_at(d, t), "feat": first + w}
                data.append(remote(block, spot, send, recv, where))
            else:
                to_worker(w, block, spot, send, recv, {})

    serve(0)
    deliver(0, 0)
    everyone[0, 0, mf] = served[0, 0]

    @pl.when(works)
    def _():
        prepare()

    pl.semaphore_wait(ready, nd - 1)
    deliver(0, 1)

    @pl.when(works)
    def _():
        for c in range(picked):
            expand(0, c)

    for d in range(1, pairs):
        serve(d)

    @pl.when(works)
    def _():
        work()

    for w, copy in loose:
        pl.when(mf != first + w)(copy.wait_send)
    for copy in data + [copy for both in wants.values() for copy in both]:
        copy.wait_send()
    for w in range(workers):
        landed(z_all.at[w], z_recv.at[w], first + w)
    for g in range(groups):
        for p in range(per):
            block = jnp.zeros((part_rows, LANES), F32)
            for q in range(per):
                value = z_all[g * per + q]
                shift = (q - p) * sub % LANES
                if shift:
                    value = pltpu.roll(value, shift, 1)
                inside = (lane >= q * sub) & (lane < (q + 1) * sub)
                block = jnp.where(inside, value, block)
            out_ref[p * part_rows : (p + 1) * part_rows, g * LANES : (g + 1) * LANES] = block

def per_device(
    nd,
    nf,
    features,
    seed_rows,
    want_rows,
    live_counts,
    hop_one,
    hop_two,
    w1_self,
    w1_neigh,
    b1,
    w2_self,
    w2_neigh,
    b2,
):
    height, nodes = features.shape
    seeds = seed_rows.shape[0]
    hid_dev = b1.shape[0]
    hid, depth = w1_self.shape
    cap = want_rows.shape[2]
    fan1 = hop_one.shape[0]
    workers = nf // 2
    columns = (fan1 + 1) * (seeds // workers)
    result = (hid_dev * (seeds // workers) // LANES, LANES)
    groups = seeds // LANES
    vmem = pl.BlockSpec(memory_space=pltpu.VMEM)
    dma = pltpu.SemaphoreType.DMA
    return pl.pallas_call(
        functools.partial(kernel, nd, nf),
        out_shape=pltpu.VMEM((hid_dev, seeds), F32),
        in_specs=[pl.BlockSpec(memory_space=pl.ANY)] * 12,
        out_specs=vmem,
        scratch_shapes=[
            pltpu.VMEM((height, nodes), BF16),
            pltpu.VMEM((1, seeds), jnp.int32),
            pltpu.SMEM((1, seeds), jnp.int32),
            pltpu.VMEM((nd, cap), jnp.int32),
            pltpu.SMEM((1, nd), jnp.int32),
            pltpu.VMEM(hop_one.shape, jnp.int32),
            pltpu.VMEM(hop_two.shape, jnp.int32),
            pltpu.VMEM((hid, 2 * depth), BF16),
            pltpu.VMEM((nd, 1, cap), jnp.int32),
            pltpu.VMEM((nd, 1, cap), jnp.int32),
            pltpu.VMEM((nd // 2, 2, 1, cap), jnp.int32),
            pltpu.SMEM((nd // 2, 2, 1, cap), jnp.int32),
            pltpu.VMEM((nodes * height // depth, LANES), F32),
            pltpu.VMEM((nd + groups, LANES, LANES), F32),
            pltpu.VMEM((nd // 2, 2, height, cap), BF16),
            pltpu.VMEM((nd // 2, 2, nf, height, cap), BF16),
            pltpu.VMEM((groups, height, LANES), BF16),
            pltpu.VMEM((nf, height, LANES), BF16),
            pltpu.VMEM((2, nf, hid_dev, w2_self.shape[0]), BF16),
            pltpu.VMEM((nf, 1, hid_dev), F32),
            pltpu.VMEM((nf, 1, hid_dev), F32),
            pltpu.VMEM((columns // LANES, 16, LANES), jnp.int32),
            pltpu.VMEM((pl.cdiv(nd, 8), LANES, columns), jnp.int32),
            pltpu.VMEM((nd * cap, columns), BF16),
            pltpu.VMEM((nd * cap, columns), BF16),
            pltpu.VMEM((depth, columns), F32),
            pltpu.VMEM((depth, columns), F32),
            pltpu.VMEM((2 * depth, columns), BF16),
            pltpu.VMEM((hid, 2 * hid), BF16),
            pltpu.VMEM((nf,) + result, F32),
            pltpu.VMEM((workers,) + result, F32),
            dma((14,)),
            pltpu.SemaphoreType.REGULAR,
        ]
        + [dma((nd // 2, 2))] * 4
        + [dma((nd // 2, 2, workers)), dma((nd // 2, 2, nf))]
        + [dma((workers,)), dma((nf,))]
        + [dma((workers, 3)), dma((nf, 3))]
        + [dma((nf,))] * 2
        + [dma((nf,)), dma((workers,))],
        compiler_params=pltpu.CompilerParams(collective_id=0, has_side_effects=True),
    )(
        features,
        seed_rows.reshape(1, seeds),
        want_rows,
        live_counts,
        hop_one,
        hop_two,
        w1_self,
        w1_neigh,
        w2_self.T,
        w2_neigh.T,
        b1.reshape(1, hid_dev),
        b2.reshape(1, hid_dev),
    )


def solution(mesh):
    return jax.shard_map(
        functools.partial(per_device, mesh.shape["dom"], mesh.shape["feat"]),
        mesh=mesh,
        in_specs=(
            P("feat", "dom"),
            P("dom"),
            P("dom", None, None),
            P("dom", None),
            P(None, "dom"),
            P(None, None, "dom"),
            P(),
            P(),
            P("feat"),
            P(None, "feat"),
            P(None, "feat"),
            P("feat"),
        ),
        out_specs=P("feat", "dom"),
        check_vma=False,
    )
```

```python
import functools

import jax
import jax.numpy as jnp
from jax import lax
from jax.experimental import pallas as pl
from jax.experimental.pallas import tpu as pltpu
from jax.sharding import PartitionSpec as P

LANES = 128
MESH = pl.DeviceIdType.MESH
BF16 = jnp.bfloat16
F32 = jnp.float32


def split_three(x):
    a = x.astype(BF16)
    rest = x - a.astype(F32)
    b = rest.astype(BF16)
    c = (rest - b.astype(F32)).astype(BF16)
    return a, b, c


def kernel(
    nd,
    nf,
    feat_hbm,
    seed_hbm,
    want_hbm,
    live_hbm,
    one_hbm,
    two_hbm,
    w1s_hbm,
    w1n_hbm,
    w2s_hbm,
    w2n_hbm,
    b1_hbm,
    b2_hbm,
    out_ref,
    feat_vm,
    seed_vm,
    seed_sm,
    want_vm,
    live_sm,
    one_ref,
    two_ref,
    w1_ref,
    asks,
    got,
    got_sm,
    table,
    rows_vm,
    served,
    everyone,
    seed_own,
    seed_all,
    w2_all,
    b_all,
    hop_rows,
    words,
    pick_one,
    pick_two,
    own_sum,
    mean_sum,
    xm_all,
    w2_full,
    z_own,
    z_all,
    local_sem,
    ready,
    want_send,
    want_recv,
    data_send,
    data_recv,
    side_send,
    side_recv,
):
    height, nodes = feat_vm.shape
    fan1, seeds = one_ref.shape
    fan2 = two_ref.shape[0]
    workers = nf // 2
    first = nf // 4
    sub = seeds // workers
    per = LANES // sub
    chunks = (fan1 + 1) * sub // LANES
    hid_dev = out_ref.shape[0]
    hid = w1_ref.shape[0]
    depth = w1_ref.shape[1] // 2
    part_rows = hid_dev // per
    groups = seeds // LANES
    pieces = depth // height
    table_rows = nodes // pieces
    me = lax.axis_index("dom")
    mf = lax.axis_index("feat")
    pairs = nd // 2
    odd = lax.rem(me, 2)
    mine = mf - first
    works = (mf >= first) & (mf < first + workers)

    def flip(x, bits):
        bit = 1
        while bit <= bits:
            if bits & bit:
                x = x + bit * (1 - 2 * lax.rem(x // bit, 2))
            bit *= 2
        return x

    def other(t):
        return odd + t * (1 - 2 * odd)

    def dom_at(d, t):
        return 2 * flip(me // 2, d) + other(t)

    def feat_at(d):
        return lax.rem(mf + d, nf)

    def local(i, src, dst):
        copy = pltpu.make_async_copy(src, dst, local_sem.at[i])
        copy.start()
        return copy

    barrier = pltpu.get_barrier_semaphore()
    for d in range(1, nf):
        pl.semaphore_signal(barrier, inc=1, device_id={"feat": feat_at(d)}, device_id_type=MESH)
    peers = [(d, t) for d in range(pairs) for t in range(2)][1:]
    for d, t in peers:
        pl.semaphore_signal(barrier, inc=1, device_id={"dom": dom_at(d, t)}, device_id_type=MESH)

    want_copies = [local(0, want_hbm.at[0], want_vm), local(1, live_hbm, live_sm)]
    feat_copy = local(2, feat_hbm, feat_vm)
    for i, (b_hbm, w2_hbm) in enumerate(((b1_hbm, w2s_hbm), (b2_hbm, w2n_hbm))):
        local(3, b_hbm, b_all.at[i, mf])
        local(4, w2_hbm, w2_all.at[i, mf])
    seed_local = [local(5, seed_hbm, seed_vm), local(6, seed_hbm, seed_sm)]
    hop_copies = [
        pltpu.make_async_copy(one_hbm, one_ref, local_sem.at[7]),
        pltpu.make_async_copy(two_hbm, two_ref, local_sem.at[8]),
    ]
    weight_copies = [
        pltpu.make_async_copy(w1s_hbm, w1_ref.at[:, :depth], local_sem.at[9]),
        pltpu.make_async_copy(w1n_hbm, w1_ref.at[:, depth:], local_sem.at[9]),
    ]

    def drain(ref, sem):
        pltpu.make_async_copy(ref, ref, sem).wait()

    @pl.when(works)
    def _():
        for copy in hop_copies + weight_copies:
            copy.start()

    def remote(src, dst, send, recv, where):
        copy = pltpu.make_async_remote_copy(
            src_ref=src,
            dst_ref=dst,
            send_sem=send,
            recv_sem=recv,
            device_id=where,
            device_id_type=MESH,
        )
        copy.start()
        return copy

    lane = lax.broadcasted_iota(jnp.int32, (1, LANES), 1)
    for copy in want_copies:
        copy.wait()
    for o in range(nd):
        wanted = jnp.where(lane < live_sm[0, o], want_vm[o : o + 1], -1)
        asks[0, o] = wanted
        asks[1, o] = wanted & (table_rows - 1)
    feat_copy.wait()
    tiles = table_rows // LANES
    step = min(8, tiles)

    def turn(i, carry):
        for u in range(step):
            t = i * step + u
            stack = jnp.concatenate(
                [
                    feat_vm[
                        :, pl.ds(pl.multiple_of(p * table_rows + t * LANES, LANES), LANES)
                    ].astype(F32)
                    for p in range(pieces)
                ],
                axis=0,
            )
            table[pl.ds(pl.multiple_of(t * LANES, LANES), LANES), :] = jnp.transpose(stack)
        return carry

    lax.fori_loop(0, tiles // step, turn, 0)

    base = pl.multiple_of(mine * sub // LANES * LANES, LANES)
    within = lax.rem(mine * sub, LANES)
    slot = lax.broadcasted_iota(jnp.int32, (LANES, LANES), 0)
    each = 8
    picked = chunks if per > 1 else chunks - 1

    @pl.when(works)
    def _():
        for copy in hop_copies:
            copy.wait()
        for k in range(fan2 + 1):
            if k < fan2:
                rows = two_ref[k, :, pl.ds(base, LANES)]
            else:
                rows = one_ref[:, pl.ds(base, LANES)]
            owner = rows >> 7
            rel = ((owner >> 1) ^ (me // 2)) * 2 + ((owner & 1) ^ odd)
            rows = (rows & (LANES - 1)) + rel * LANES
            turned = [
                pltpu.roll(rows, lax.rem(q * sub - within + LANES, LANES), 1) for q in range(per)
            ]
            for c in range(chunks):
                row = jnp.full((1, LANES), -1, jnp.int32)
                for q in range(per):
                    j = c * per + q
                    if j < fan1:
                        inside = (lane >= q * sub) & (lane < (q + 1) * sub)
                        row = jnp.where(inside, turned[q][j : j + 1], row)
                hop_rows[c, k : k + 1, :] = row

    pl.semaphore_wait(barrier, nd + nf - 2)

    for d, t in peers:
        pl.semaphore_signal(ready, inc=1, device_id={"dom": dom_at(d, t)}, device_id_type=MESH)
    for d, t in peers:
        where = {"dom": dom_at(d, t)}
        to = dom_at(d, t)
        remote(asks.at[0, to], got.at[d, t], want_send.at[0], want_recv.at[0, d], where)
        remote(asks.at[1, to], got_sm.at[d, t], want_send.at[1], want_recv.at[1, d], where)
    own_sm = local(10, asks.at[1, me], got_sm.at[0, 0])
    got[0, 0] = asks[0, me]
    drain(b_all.at[:, mf], local_sem.at[3])
    drain(w2_all.at[:, mf], local_sem.at[4])
    buddy = {"dom": dom_at(0, 1)}

    def to_worker(w, src, dst, send, recv, where):
        copy = pltpu.make_async_remote_copy(
            src_ref=src,
            dst_ref=dst,
            send_sem=send,
            recv_sem=recv,
            device_id={**where, "feat": first + w},
            device_id_type=MESH,
        )
        pl.when(mf != first + w)(copy.start)

    for w in range(workers):
        for ref, i in ((b_all.at[0, mf], 0), (b_all.at[1, mf], 0), (w2_all.at[odd, mf], 1)):
            to_worker(w, ref, ref, side_send.at[i], side_recv.at[i], {})

    def gather(jobs):
        for slot, read, _ in jobs:
            for k in range(LANES):
                rows_vm[slot, k : k + 1, :] = table[pl.ds(read(k), 1), :]
        blocks = []
        for slot, _, wanted in jobs:
            turned = jnp.transpose(rows_vm[slot])
            piece = wanted >> (table_rows.bit_length() - 1)
            block = jnp.zeros((height, LANES), F32)
            for p in range(pieces):
                block = jnp.where(piece == p, turned[p * height : (p + 1) * height], block)
            blocks.append(block.astype(BF16))
        return blocks

    for copy in seed_local:
        copy.wait()
    def seed_job(g):
        at = g * LANES
        return (
            nd + g,
            lambda k: seed_sm[0, at + k] & (table_rows - 1),
            seed_vm[:, at : at + LANES],
        )

    for g, block in enumerate(gather([seed_job(g) for g in range(groups)])):
        seed_own[g] = block
    for w in range(workers):
        block = seed_own.at[w * sub // LANES]
        to_worker(w, block, seed_all.at[mf], side_send.at[2], side_recv.at[2], {})

    @pl.when(works)
    def _():
        seed_all[mf] = seed_own[mine * sub // LANES]

    steps = min(4, pairs)
    ends = [nd * i // steps for i in range(steps + 1)]

    def expand(i, c):
        columns = slice(c * LANES, (c + 1) * LANES)
        short = jnp.int16
        row = jnp.broadcast_to(hop_rows[c, fan2 : fan2 + 1, :], (16, LANES)).astype(short)
        row = jnp.concatenate([row] * (LANES // 16), axis=0)
        for o in range(ends[i], ends[i + 1]):
            these = slice(o * LANES, (o + 1) * LANES)
            count = lax.shift_right_logical(words[o // each, :, columns], o % each * 4) & 15
            pick_two[these, columns] = count.astype(F32).astype(BF16)
            same = row == (slot + o * LANES).astype(short)
            pick_one[these, columns] = jnp.where(same, jnp.ones((), BF16), jnp.zeros((), BF16))

    def prepare():
        for c in range(picked):
            columns = slice(c * LANES, (c + 1) * LANES)
            for g in range(words.shape[0]):
                count = jnp.zeros((LANES, LANES), jnp.int32)
                for k in range(fan2):
                    row = hop_rows[c, k : k + 1, :]
                    rel = (row >> 7) - g * each
                    real = (row >= 0) & (rel >= 0) & (rel < each)
                    unit = jnp.where(real, jnp.left_shift(1, (rel & (each - 1)) * 4), 0)
                    count = count + jnp.where((row & (LANES - 1)) == slot, unit, 0)
                words[g, :, columns] = count
        for c in range(picked):
            expand(0, c)

    def work():
        drain(b_all.at[:, : nf - 1], side_recv.at[0])
        drain(w2_all.at[0, : nf - 1], side_recv.at[1])
        for d in range(1, nf):
            ref = w2_all.at[odd, feat_at(d)]
            remote(ref, ref, side_send.at[4], side_recv.at[3], buddy)

        def column(rows):
            return jnp.concatenate(
                [jnp.transpose(jnp.broadcast_to(rows[f], (LANES, hid_dev))) for f in range(nf)], axis=0
            )

        b1 = column(b_all[0])
        b2 = column(b_all[1])
        for c in range(picked if steps > 1 else 0):
            expand(1, c)
        drain(seed_all.at[: nf - 1], side_recv.at[2])

        def whole(blocks):
            if height % 16:
                return blocks.astype(F32).reshape(depth, LANES).astype(BF16)
            return blocks.reshape(depth, LANES)

        x_seed = whole(seed_all[...]).astype(F32)
        if per > 1:
            x_seed = pltpu.roll(x_seed, lax.rem(2 * LANES - sub - within, LANES), 1)

        wide = 2 * LANES
        total = jnp.zeros((depth, LANES), F32)
        done = 0
        for i in range(steps):
            part = [(o // 2, o % 2) for o in range(ends[i], ends[i + 1])]
            if i == 1:
                for later in range(2, steps):
                    for c in range(picked):
                        expand(later, c)
                drain(w1_ref, local_sem.at[9])
                drain(w2_all.at[0, : nf - 1], side_recv.at[3])
                w2_full[...] = jnp.transpose(w2_all[...].reshape(2 * hid, w2_all.shape[3]))
            for d in range(ends[i] // 2, ends[i + 1] // 2):
                if d:
                    drain(everyone.at[d], data_recv.at[d])
                else:
                    drain(everyone.at[0, 0, : nf - 1], data_recv.at[0])
                    drain(everyone.at[0, 1], data_recv.at[pairs])
            fetched = jnp.concatenate([whole(everyone[d, t]) for d, t in part], axis=1)
            these = slice(done, done + len(part) * LANES)
            done += len(part) * LANES
            for n in range(0, picked, 2):
                columns = slice(n * LANES, min(n + 2, picked) * LANES)
                own = jnp.dot(fetched, pick_one[these, columns], preferred_element_type=F32)
                mean = jnp.dot(fetched, pick_two[these, columns], preferred_element_type=F32)
                if i:
                    own = own + own_sum[:, columns]
                    mean = mean + mean_sum[:, columns]
                if i < steps - 1:
                    own_sum[:, columns] = own
                    mean_sum[:, columns] = mean
                    continue
                for at in range(0, own.shape[1], LANES):
                    total = total + own[:, at : at + LANES]
                xm_all[:depth, columns] = own.astype(BF16)
                xm_all[depth:, columns] = (mean * (1.0 / fan2)).astype(BF16)

        def fold(value):
            width = sub
            while width < LANES:
                value = value + pltpu.roll(value, width, 1)
                width *= 2
            return value

        is_seed = lane >= LANES - sub
        last = slice((chunks - 1) * LANES, chunks * LANES)
        m_one = fold(total) * (1.0 / fan1)
        if per > 1:
            x_seed = jnp.where(is_seed, x_seed, xm_all[:depth, last].astype(F32))
            m_one = jnp.where(is_seed, m_one, xm_all[depth:, last].astype(F32))
        xm_all[:depth, last] = x_seed.astype(BF16)
        xm_all[depth:, last] = m_one.astype(BF16)

        total = jnp.zeros((hid, LANES), F32)
        for n in range(chunks * LANES // wide):
            columns = slice(n * wide, (n + 1) * wide)
            pre = jnp.dot(w1_ref[...], xm_all[:, columns], preferred_element_type=F32)
            left = jnp.maximum(pre[:, :LANES] + b1, 0.0)
            right = jnp.maximum(pre[:, LANES:] + b1, 0.0)
            if n == chunks * LANES // wide - 1:
                h_seed = right
                right = jnp.where(is_seed, 0.0, right)
            total = total + left + right
        g_mean = fold(total) * (1.0 / fan1)
        stacked = jnp.concatenate([h_seed, g_mean], axis=0)
        z = jnp.zeros((hid, LANES), F32)
        for term in reversed(split_three(stacked)):
            z = z + jnp.dot(w2_full[...], term, preferred_element_type=F32)
        z = z + b2
        square = jnp.sum(z * z, axis=0, keepdims=True)
        z = z * lax.rsqrt(square * (1.0 / hid) + 1.0)
        for f in range(nf):
            packed = jnp.zeros((part_rows, LANES), F32)
            for p in range(per):
                row = f * hid_dev + p * part_rows
                value = z[row : row + part_rows]
                shift = (p * sub + sub) % LANES
                if shift:
                    value = pltpu.roll(value, shift, 1)
                packed = jnp.where((lane >= p * sub) & (lane < (p + 1) * sub), value, packed)
            z_own[f] = packed

        for e in range(1, nf):
            to = feat_at(e)
            where = {"feat": to}
            remote(z_own.at[to], z_all.at[mine], side_send.at[5], side_recv.at[4], where)
        z_all[mine] = z_own[mf]

    def want_job(d, t):
        return (2 * d + t, lambda k: got_sm[d, t, 0, k], got[d, t])

    def arrived(d, these):
        for i, ref in enumerate((got, got_sm)):
            pltpu.make_async_remote_copy(
                src_ref=asks.at[i, these],
                dst_ref=ref.at[d, these],
                send_sem=want_send.at[i],
                recv_sem=want_recv.at[i, d],
                device_id=buddy,
                device_id_type=MESH,
            ).wait_recv()

    def deliver(d, t):
        for w in range(workers):
            block = served.at[d, t]
            spot = everyone.at[d, t, mf]
            if d or t:
                where = {"dom": dom_at(d, t), "feat": first + w}
                remote(block, spot, data_send.at[min(d, 1)], data_recv.at[d or pairs], where)
            else:
                to_worker(w, block, spot, side_send.at[3], data_recv.at[0], {})

    own_sm.wait()
    served[0, 0] = gather([want_job(0, 0)])[0]
    deliver(0, 0)
    everyone[0, 0, mf] = served[0, 0]

    @pl.when(works)
    def _():
        prepare()

    arrived(0, slice(1, 2))
    served[0, 1] = gather([want_job(0, 1)])[0]
    pl.semaphore_wait(ready, nd - 1)
    deliver(0, 1)
    for d in range(1, pairs):
        arrived(d, slice(0, 2))
        for t, block in enumerate(gather([want_job(d, t) for t in range(2)])):
            served[d, t] = block
            deliver(d, t)

    @pl.when(works)
    def _():
        work()

    def sent(n):
        drain(b_all.at[:, :n], side_send.at[0])
        drain(w2_all.at[0, :n], side_send.at[1])
        drain(seed_all.at[:n], side_send.at[2])
        drain(everyone.at[0, 0, :n], side_send.at[3])

    drain(asks.at[0, : nd - 1], want_send.at[0])
    drain(asks.at[1, : nd - 1], want_send.at[1])
    drain(everyone.at[0, 1, :workers], data_send.at[0])
    drain(everyone.at[1:, :, :workers], data_send.at[1])

    @pl.when(works)
    def _():
        sent(workers - 1)
        drain(w2_all.at[0, : nf - 1], side_send.at[4])
        drain(z_own.at[: nf - 1], side_send.at[5])
        drain(z_all.at[: workers - 1], side_recv.at[4])

    @pl.when(jnp.logical_not(works))
    def _():
        sent(workers)
        drain(z_all, side_recv.at[4])

    for g in range(groups):
        for p in range(per):
            block = jnp.zeros((part_rows, LANES), F32)
            for q in range(per):
                value = z_all[g * per + q]
                shift = (q - p) * sub % LANES
                if shift:
                    value = pltpu.roll(value, shift, 1)
                inside = (lane >= q * sub) & (lane < (q + 1) * sub)
                block = jnp.where(inside, value, block)
            out_ref[p * part_rows : (p + 1) * part_rows, g * LANES : (g + 1) * LANES] = block

def per_device(
    nd,
    nf,
    features,
    seed_rows,
    want_rows,
    live_counts,
    hop_one,
    hop_two,
    w1_self,
    w1_neigh,
    b1,
    w2_self,
    w2_neigh,
    b2,
):
    height, nodes = features.shape
    seeds = seed_rows.shape[0]
    hid_dev = b1.shape[0]
    hid, depth = w1_self.shape
    cap = want_rows.shape[2]
    fan1 = hop_one.shape[0]
    workers = nf // 2
    columns = (fan1 + 1) * (seeds // workers)
    result = (hid_dev * (seeds // workers) // LANES, LANES)
    groups = seeds // LANES
    vmem = pl.BlockSpec(memory_space=pltpu.VMEM)
    dma = pltpu.SemaphoreType.DMA
    return pl.pallas_call(
        functools.partial(kernel, nd, nf),
        out_shape=pltpu.VMEM((hid_dev, seeds), F32),
        in_specs=[pl.BlockSpec(memory_space=pl.ANY)] * 12,
        out_specs=vmem,
        scratch_shapes=[
            pltpu.VMEM((height, nodes), BF16),
            pltpu.VMEM((1, seeds), jnp.int32),
            pltpu.SMEM((1, seeds), jnp.int32),
            pltpu.VMEM((nd, cap), jnp.int32),
            pltpu.SMEM((1, nd), jnp.int32),
            pltpu.VMEM(hop_one.shape, jnp.int32),
            pltpu.VMEM(hop_two.shape, jnp.int32),
            pltpu.VMEM((hid, 2 * depth), BF16),
            pltpu.VMEM((2, nd, 1, cap), jnp.int32),
            pltpu.VMEM((nd // 2, 2, 1, cap), jnp.int32),
            pltpu.SMEM((nd // 2, 2, 1, cap), jnp.int32),
            pltpu.VMEM((nodes * height // depth, LANES), F32),
            pltpu.VMEM((nd + groups, LANES, LANES), F32),
            pltpu.VMEM((nd // 2, 2, height, cap), BF16),
            pltpu.VMEM((nd // 2, 2, nf, height, cap), BF16),
            pltpu.VMEM((groups, height, LANES), BF16),
            pltpu.VMEM((nf, height, LANES), BF16),
            pltpu.VMEM((2, nf, hid_dev, w2_self.shape[0]), BF16),
            pltpu.VMEM((2, nf, 1, hid_dev), F32),
            pltpu.VMEM((columns // LANES, 16, LANES), jnp.int32),
            pltpu.VMEM((pl.cdiv(nd, 8), LANES, columns), jnp.int32),
            pltpu.VMEM((nd * cap, columns), BF16),
            pltpu.VMEM((nd * cap, columns), BF16),
            pltpu.VMEM((depth, columns), F32),
            pltpu.VMEM((depth, columns), F32),
            pltpu.VMEM((2 * depth, columns), BF16),
            pltpu.VMEM((hid, 2 * hid), BF16),
            pltpu.VMEM((nf,) + result, F32),
            pltpu.VMEM((workers,) + result, F32),
            dma((11,)),
            pltpu.SemaphoreType.REGULAR,
            dma((2,)),
            dma((2, nd // 2)),
            dma((2,)),
            dma((nd // 2 + 1,)),
            dma((6,)),
            dma((5,)),
        ],
        compiler_params=pltpu.CompilerParams(collective_id=0, has_side_effects=True),
    )(
        features,
        seed_rows.reshape(1, seeds),
        want_rows,
        live_counts,
        hop_one,
        hop_two,
        w1_self,
        w1_neigh,
        w2_self.T,
        w2_neigh.T,
        b1.reshape(1, hid_dev),
        b2.reshape(1, hid_dev),
    )


def solution(mesh):
    return jax.shard_map(
        functools.partial(per_device, mesh.shape["dom"], mesh.shape["feat"]),
        mesh=mesh,
        in_specs=(
            P("feat", "dom"),
            P("dom"),
            P("dom", None, None),
            P("dom", None),
            P(None, "dom"),
            P(None, None, "dom"),
            P(),
            P(),
            P("feat"),
            P(None, "feat"),
            P(None, "feat"),
            P("feat"),
        ),
        out_specs=P("feat", "dom"),
        check_vma=False,
    )
```

```python
import functools

import jax
import jax.numpy as jnp
from jax import lax
from jax.experimental import pallas as pl
from jax.experimental.pallas import tpu as pltpu
from jax.sharding import PartitionSpec as P

LANES = 128
MESH = pl.DeviceIdType.MESH
BF16 = jnp.bfloat16
F32 = jnp.float32


def split_three(x):
    a = x.astype(BF16)
    rest = x - a.astype(F32)
    b = rest.astype(BF16)
    c = (rest - b.astype(F32)).astype(BF16)
    return a, b, c


def kernel(
    nd,
    nf,
    feat_hbm,
    seed_hbm,
    want_hbm,
    live_hbm,
    one_hbm,
    two_hbm,
    w1s_hbm,
    w1n_hbm,
    w2s_hbm,
    w2n_hbm,
    b1_hbm,
    b2_hbm,
    out_ref,
    feat_vm,
    seed_vm,
    seed_sm,
    want_vm,
    live_sm,
    one_ref,
    two_ref,
    w1_ref,
    asks,
    got,
    got_sm,
    table,
    rows_vm,
    served,
    everyone,
    seed_own,
    seed_all,
    w2_all,
    b_all,
    hop_rows,
    words,
    pick_one,
    pick_two,
    own_sum,
    mean_sum,
    xm_all,
    w2_full,
    z_own,
    z_all,
    local_sem,
    ready,
    want_send,
    want_recv,
    data_send,
    data_recv,
    side_send,
    side_recv,
):
    height, nodes = feat_vm.shape
    fan1, seeds = one_ref.shape
    fan2 = two_ref.shape[0]
    workers = nf // 2
    first = nf // 4
    sub = seeds // workers
    per = LANES // sub
    chunks = (fan1 + 1) * sub // LANES
    hid_dev = out_ref.shape[0]
    hid = w1_ref.shape[0]
    depth = w1_ref.shape[1] // 2
    part_rows = hid_dev // per
    groups = seeds // LANES
    pieces = depth // height
    table_rows = nodes // pieces
    me = lax.axis_index("dom")
    mf = lax.axis_index("feat")
    pairs = nd // 2
    odd = lax.rem(me, 2)
    mine = mf - first
    works = (mf >= first) & (mf < first + workers)

    def flip(x, bits):
        bit = 1
        while bit <= bits:
            if bits & bit:
                x = x + bit * (1 - 2 * lax.rem(x // bit, 2))
            bit *= 2
        return x

    def other(t):
        return odd + t * (1 - 2 * odd)

    def dom_at(d, t):
        return 2 * flip(me // 2, d) + other(t)

    def feat_at(d):
        return lax.rem(mf + d, nf)

    def local(i, src, dst):
        copy = pltpu.make_async_copy(src, dst, local_sem.at[i])
        copy.start()
        return copy

    barrier = pltpu.get_barrier_semaphore()
    for d in range(1, nf):
        pl.semaphore_signal(barrier, inc=1, device_id={"feat": feat_at(d)}, device_id_type=MESH)
    peers = [(d, t) for d in range(pairs) for t in range(2)][1:]
    for d, t in peers:
        pl.semaphore_signal(barrier, inc=1, device_id={"dom": dom_at(d, t)}, device_id_type=MESH)

    want_copies = [local(0, want_hbm.at[0], want_vm), local(1, live_hbm, live_sm)]
    feat_copy = local(2, feat_hbm, feat_vm)
    for i, (b_hbm, w2_hbm) in enumerate(((b1_hbm, w2s_hbm), (b2_hbm, w2n_hbm))):
        local(3, b_hbm, b_all.at[i, mf])
        local(4, w2_hbm, w2_all.at[i, mf])
    seed_local = [local(5, seed_hbm, seed_vm), local(6, seed_hbm, seed_sm)]
    hop_copies = [
        pltpu.make_async_copy(one_hbm, one_ref, local_sem.at[7]),
        pltpu.make_async_copy(two_hbm, two_ref, local_sem.at[8]),
    ]
    weight_copies = [
        pltpu.make_async_copy(w1s_hbm, w1_ref.at[:, :depth], local_sem.at[9]),
        pltpu.make_async_copy(w1n_hbm, w1_ref.at[:, depth:], local_sem.at[9]),
    ]

    def drain(ref, sem):
        pltpu.make_async_copy(ref, ref, sem).wait()

    @pl.when(works)
    def _():
        for copy in hop_copies + weight_copies:
            copy.start()

    def remote(src, dst, send, recv, where):
        copy = pltpu.make_async_remote_copy(
            src_ref=src,
            dst_ref=dst,
            send_sem=send,
            recv_sem=recv,
            device_id=where,
            device_id_type=MESH,
        )
        copy.start()
        return copy

    lane = lax.broadcasted_iota(jnp.int32, (1, LANES), 1)
    for copy in want_copies:
        copy.wait()
    for o in range(nd):
        wanted = jnp.where(lane < live_sm[0, o], want_vm[o : o + 1], -1)
        asks[0, o] = wanted
        asks[1, o] = wanted & (table_rows - 1)
    feat_copy.wait()
    tiles = table_rows // LANES
    step = min(8, tiles)

    def turn(i, carry):
        for u in range(step):
            t = i * step + u
            stack = jnp.concatenate(
                [
                    feat_vm[
                        :, pl.ds(pl.multiple_of(p * table_rows + t * LANES, LANES), LANES)
                    ].astype(F32)
                    for p in range(pieces)
                ],
                axis=0,
            )
            table[pl.ds(pl.multiple_of(t * LANES, LANES), LANES), :] = jnp.transpose(stack)
        return carry

    lax.fori_loop(0, tiles // step, turn, 0)

    pl.semaphore_wait(barrier, nd + nf - 2)

    for d, t in peers:
        pl.semaphore_signal(ready, inc=1, device_id={"dom": dom_at(d, t)}, device_id_type=MESH)
    for d, t in peers:
        where = {"dom": dom_at(d, t)}
        to = dom_at(d, t)
        remote(asks.at[0, to], got.at[d, t], want_send.at[0], want_recv.at[0, d], where)
        remote(asks.at[1, to], got_sm.at[d, t], want_send.at[1], want_recv.at[1, d], where)
    own_sm = local(10, asks.at[1, me], got_sm.at[0, 0])
    got[0, 0] = asks[0, me]
    drain(b_all.at[:, mf], local_sem.at[3])
    drain(w2_all.at[:, mf], local_sem.at[4])
    buddy = {"dom": dom_at(0, 1)}

    def to_worker(w, src, dst, send, recv, where):
        copy = pltpu.make_async_remote_copy(
            src_ref=src,
            dst_ref=dst,
            send_sem=send,
            recv_sem=recv,
            device_id={**where, "feat": first + w},
            device_id_type=MESH,
        )
        pl.when(mf != first + w)(copy.start)

    for w in range(workers):
        for ref, i in ((b_all.at[0, mf], 0), (b_all.at[1, mf], 0), (w2_all.at[odd, mf], 1)):
            to_worker(w, ref, ref, side_send.at[i], side_recv.at[i], {})

    def gather(jobs):
        for slot, read, _ in jobs:
            for k in range(LANES):
                rows_vm[slot, k : k + 1, :] = table[pl.ds(read(k), 1), :]
        blocks = []
        for slot, _, wanted in jobs:
            turned = jnp.transpose(rows_vm[slot])
            piece = wanted >> (table_rows.bit_length() - 1)
            block = jnp.zeros((height, LANES), F32)
            for p in range(pieces):
                block = jnp.where(piece == p, turned[p * height : (p + 1) * height], block)
            blocks.append(block.astype(BF16))
        return blocks

    for copy in seed_local:
        copy.wait()
    def seed_job(g):
        at = g * LANES
        return (
            nd + g,
            lambda k: seed_sm[0, at + k] & (table_rows - 1),
            seed_vm[:, at : at + LANES],
        )

    for g, block in enumerate(gather([seed_job(g) for g in range(groups)])):
        seed_own[g] = block
    for w in range(workers):
        block = seed_own.at[w * sub // LANES]
        to_worker(w, block, seed_all.at[mf], side_send.at[2], side_recv.at[2], {})

    @pl.when(works)
    def _():
        seed_all[mf] = seed_own[mine * sub // LANES]

    base = pl.multiple_of(mine * sub // LANES * LANES, LANES)
    within = lax.rem(mine * sub, LANES)
    slot = lax.broadcasted_iota(jnp.int32, (LANES, LANES), 0)
    each = 8
    picked = chunks if per > 1 else chunks - 1
    steps = min(4, pairs)
    ends = [nd * i // steps for i in range(steps + 1)]

    def expand(owners, c):
        columns = slice(c * LANES, (c + 1) * LANES)
        short = jnp.int16
        row = jnp.broadcast_to(hop_rows[c, fan2 : fan2 + 1, :], (16, LANES)).astype(short)
        row = jnp.concatenate([row] * (LANES // 16), axis=0)
        for o in owners:
            these = slice(o * LANES, (o + 1) * LANES)
            count = lax.shift_right_logical(words[o // each, :, columns], o % each * 4) & 15
            pick_two[these, columns] = count.astype(F32).astype(BF16)
            same = row == (slot + o * LANES).astype(short)
            pick_one[these, columns] = jnp.where(same, jnp.ones((), BF16), jnp.zeros((), BF16))

    def prepare():
        for copy in hop_copies:
            copy.wait()
        for k in range(fan2 + 1):
            if k < fan2:
                rows = two_ref[k, :, pl.ds(base, LANES)]
            else:
                rows = one_ref[:, pl.ds(base, LANES)]
            owner = rows >> 7
            rel = ((owner >> 1) ^ (me // 2)) * 2 + ((owner & 1) ^ odd)
            rows = (rows & (LANES - 1)) + rel * LANES
            turned = [
                pltpu.roll(rows, lax.rem(q * sub - within + LANES, LANES), 1) for q in range(per)
            ]
            for c in range(chunks):
                row = jnp.full((1, LANES), -1, jnp.int32)
                for q in range(per):
                    j = c * per + q
                    if j < fan1:
                        inside = (lane >= q * sub) & (lane < (q + 1) * sub)
                        row = jnp.where(inside, turned[q][j : j + 1], row)
                hop_rows[c, k : k + 1, :] = row
        for c in range(picked):
            columns = slice(c * LANES, (c + 1) * LANES)
            for g in range(words.shape[0]):
                count = jnp.zeros((LANES, LANES), jnp.int32)
                for k in range(fan2):
                    row = hop_rows[c, k : k + 1, :]
                    rel = (row >> 7) - g * each
                    real = (row >= 0) & (rel >= 0) & (rel < each)
                    unit = jnp.where(real, jnp.left_shift(1, (rel & (each - 1)) * 4), 0)
                    count = count + jnp.where((row & (LANES - 1)) == slot, unit, 0)
                words[g, :, columns] = count

    def work():
        for c in range(picked):
            expand(range(ends[1]), c)
        drain(b_all.at[:, : nf - 1], side_recv.at[0])
        drain(w2_all.at[0, : nf - 1], side_recv.at[1])
        for d in range(1, nf):
            ref = w2_all.at[odd, feat_at(d)]
            remote(ref, ref, side_send.at[4], side_recv.at[3], buddy)

        def column(rows):
            return jnp.concatenate(
                [jnp.transpose(jnp.broadcast_to(rows[f], (LANES, hid_dev))) for f in range(nf)], axis=0
            )

        b1 = column(b_all[0])
        b2 = column(b_all[1])
        for c in range(picked):
            expand(range(ends[1], ends[2]), c)
        for c in range(picked):
            expand(range(ends[2], nd), c)
        drain(w1_ref, local_sem.at[9])
        drain(w2_all.at[0, : nf - 1], side_recv.at[3])
        w2_full[...] = jnp.transpose(w2_all[...].reshape(2 * hid, w2_all.shape[3]))
        drain(seed_all.at[: nf - 1], side_recv.at[2])

        def whole(blocks):
            if height % 16:
                return blocks.astype(F32).reshape(depth, LANES).astype(BF16)
            return blocks.reshape(depth, LANES)

        x_seed = whole(seed_all[...]).astype(F32)
        if per > 1:
            x_seed = pltpu.roll(x_seed, lax.rem(2 * LANES - sub - within, LANES), 1)

        def fold(value):
            width = sub
            while width < LANES:
                value = value + pltpu.roll(value, width, 1)
                width *= 2
            return value

        def layer(n):
            columns = slice(n * LANES, (n + 2) * LANES)
            pre = jnp.dot(w1_ref[...], xm_all[:, columns], preferred_element_type=F32)
            return jnp.maximum(pre[:, :LANES] + b1, 0.0), jnp.maximum(pre[:, LANES:] + b1, 0.0)

        total = jnp.zeros((depth, LANES), F32)
        summed = jnp.zeros((hid, LANES), F32)
        done = 0
        for i in range(steps):
            part = [(o // 2, o % 2) for o in range(ends[i], ends[i + 1])]
            for d in range(ends[i] // 2, ends[i + 1] // 2):
                if d:
                    drain(everyone.at[d], data_recv.at[d])
                else:
                    drain(everyone.at[0, 0, : nf - 1], data_recv.at[0])
                    drain(everyone.at[0, 1], data_recv.at[pairs])
            fetched = jnp.concatenate([whole(everyone[d, t]) for d, t in part], axis=1)
            these = slice(done, done + len(part) * LANES)
            done += len(part) * LANES
            for n in range(0, picked, 2):
                columns = slice(n * LANES, min(n + 2, picked) * LANES)
                own = jnp.dot(fetched, pick_one[these, columns], preferred_element_type=F32)
                mean = jnp.dot(fetched, pick_two[these, columns], preferred_element_type=F32)
                if i:
                    own = own + own_sum[:, columns]
                    mean = mean + mean_sum[:, columns]
                if i < steps - 1:
                    own_sum[:, columns] = own
                    mean_sum[:, columns] = mean
                    continue
                for at in range(0, own.shape[1], LANES):
                    total = total + own[:, at : at + LANES]
                xm_all[:depth, columns] = own.astype(BF16)
                xm_all[depth:, columns] = (mean * (1.0 / fan2)).astype(BF16)

        is_seed = lane >= LANES - sub
        last = slice((chunks - 1) * LANES, chunks * LANES)
        m_one = fold(total) * (1.0 / fan1)
        if per > 1:
            x_seed = jnp.where(is_seed, x_seed, xm_all[:depth, last].astype(F32))
            m_one = jnp.where(is_seed, m_one, xm_all[depth:, last].astype(F32))
        xm_all[:depth, last] = x_seed.astype(BF16)
        xm_all[depth:, last] = m_one.astype(BF16)

        for n in range(0, chunks - 2, 2):
            left, right = layer(n)
            summed = summed + left + right
        left, h_seed = layer(chunks - 2)
        summed = summed + left + jnp.where(is_seed, 0.0, h_seed)
        g_mean = fold(summed) * (1.0 / fan1)
        stacked = jnp.concatenate([h_seed, g_mean], axis=0)
        z = jnp.zeros((hid, LANES), F32)
        for term in reversed(split_three(stacked)):
            z = z + jnp.dot(w2_full[...], term, preferred_element_type=F32)
        z = z + b2
        square = jnp.sum(z * z, axis=0, keepdims=True)
        z = z * lax.rsqrt(square * (1.0 / hid) + 1.0)
        for f in range(nf):
            packed = jnp.zeros((part_rows, LANES), F32)
            for p in range(per):
                row = f * hid_dev + p * part_rows
                value = z[row : row + part_rows]
                shift = (p * sub + sub) % LANES
                if shift:
                    value = pltpu.roll(value, shift, 1)
                packed = jnp.where((lane >= p * sub) & (lane < (p + 1) * sub), value, packed)
            z_own[f] = packed

        for e in range(1, nf):
            to = feat_at(e)
            where = {"feat": to}
            remote(z_own.at[to], z_all.at[mine], side_send.at[5], side_recv.at[4], where)
        z_all[mine] = z_own[mf]

    def want_job(d, t):
        return (2 * d + t, lambda k: got_sm[d, t, 0, k], got[d, t])

    def arrived(d, these):
        for i, ref in enumerate((got, got_sm)):
            pltpu.make_async_remote_copy(
                src_ref=asks.at[i, these],
                dst_ref=ref.at[d, these],
                send_sem=want_send.at[i],
                recv_sem=want_recv.at[i, d],
                device_id=buddy,
                device_id_type=MESH,
            ).wait_recv()

    def deliver(d, t):
        for w in range(workers):
            block = served.at[d, t]
            spot = everyone.at[d, t, mf]
            if d or t:
                where = {"dom": dom_at(d, t), "feat": first + w}
                remote(block, spot, data_send.at[min(d, 1)], data_recv.at[d or pairs], where)
            else:
                to_worker(w, block, spot, side_send.at[3], data_recv.at[0], {})

    own_sm.wait()
    served[0, 0] = gather([want_job(0, 0)])[0]
    deliver(0, 0)
    everyone[0, 0, mf] = served[0, 0]

    @pl.when(works)
    def _():
        prepare()

    arrived(0, slice(1, 2))
    served[0, 1] = gather([want_job(0, 1)])[0]
    pl.semaphore_wait(ready, nd - 1)
    deliver(0, 1)
    for d in range(1, pairs):
        arrived(d, slice(0, 2))
        for t, block in enumerate(gather([want_job(d, t) for t in range(2)])):
            served[d, t] = block
            deliver(d, t)

    @pl.when(works)
    def _():
        work()

    def sent(n):
        drain(b_all.at[:, :n], side_send.at[0])
        drain(w2_all.at[0, :n], side_send.at[1])
        drain(seed_all.at[:n], side_send.at[2])
        drain(everyone.at[0, 0, :n], side_send.at[3])

    drain(asks.at[0, : nd - 1], want_send.at[0])
    drain(asks.at[1, : nd - 1], want_send.at[1])
    drain(everyone.at[0, 1, :workers], data_send.at[0])
    drain(everyone.at[1:, :, :workers], data_send.at[1])

    @pl.when(works)
    def _():
        sent(workers - 1)
        drain(w2_all.at[0, : nf - 1], side_send.at[4])
        drain(z_own.at[: nf - 1], side_send.at[5])
        drain(z_all.at[: workers - 1], side_recv.at[4])

    @pl.when(jnp.logical_not(works))
    def _():
        sent(workers)
        drain(z_all, side_recv.at[4])

    for g in range(groups):
        for p in range(per):
            block = jnp.zeros((part_rows, LANES), F32)
            for q in range(per):
                value = z_all[g * per + q]
                shift = (q - p) * sub % LANES
                if shift:
                    value = pltpu.roll(value, shift, 1)
                inside = (lane >= q * sub) & (lane < (q + 1) * sub)
                block = jnp.where(inside, value, block)
            out_ref[p * part_rows : (p + 1) * part_rows, g * LANES : (g + 1) * LANES] = block

def per_device(
    nd,
    nf,
    features,
    seed_rows,
    want_rows,
    live_counts,
    hop_one,
    hop_two,
    w1_self,
    w1_neigh,
    b1,
    w2_self,
    w2_neigh,
    b2,
):
    height, nodes = features.shape
    seeds = seed_rows.shape[0]
    hid_dev = b1.shape[0]
    hid, depth = w1_self.shape
    cap = want_rows.shape[2]
    fan1 = hop_one.shape[0]
    workers = nf // 2
    columns = (fan1 + 1) * (seeds // workers)
    result = (hid_dev * (seeds // workers) // LANES, LANES)
    groups = seeds // LANES
    vmem = pl.BlockSpec(memory_space=pltpu.VMEM)
    dma = pltpu.SemaphoreType.DMA
    return pl.pallas_call(
        functools.partial(kernel, nd, nf),
        out_shape=pltpu.VMEM((hid_dev, seeds), F32),
        in_specs=[pl.BlockSpec(memory_space=pl.ANY)] * 12,
        out_specs=vmem,
        scratch_shapes=[
            pltpu.VMEM((height, nodes), BF16),
            pltpu.VMEM((1, seeds), jnp.int32),
            pltpu.SMEM((1, seeds), jnp.int32),
            pltpu.VMEM((nd, cap), jnp.int32),
            pltpu.SMEM((1, nd), jnp.int32),
            pltpu.VMEM(hop_one.shape, jnp.int32),
            pltpu.VMEM(hop_two.shape, jnp.int32),
            pltpu.VMEM((hid, 2 * depth), BF16),
            pltpu.VMEM((2, nd, 1, cap), jnp.int32),
            pltpu.VMEM((nd // 2, 2, 1, cap), jnp.int32),
            pltpu.SMEM((nd // 2, 2, 1, cap), jnp.int32),
            pltpu.VMEM((nodes * height // depth, LANES), F32),
            pltpu.VMEM((nd + groups, LANES, LANES), F32),
            pltpu.VMEM((nd // 2, 2, height, cap), BF16),
            pltpu.VMEM((nd // 2, 2, nf, height, cap), BF16),
            pltpu.VMEM((groups, height, LANES), BF16),
            pltpu.VMEM((nf, height, LANES), BF16),
            pltpu.VMEM((2, nf, hid_dev, w2_self.shape[0]), BF16),
            pltpu.VMEM((2, nf, 1, hid_dev), F32),
            pltpu.VMEM((columns // LANES, 16, LANES), jnp.int32),
            pltpu.VMEM((pl.cdiv(nd, 8), LANES, columns), jnp.int32),
            pltpu.VMEM((nd * cap, columns), BF16),
            pltpu.VMEM((nd * cap, columns), BF16),
            pltpu.VMEM((depth, columns), F32),
            pltpu.VMEM((depth, columns), F32),
            pltpu.VMEM((2 * depth, columns), BF16),
            pltpu.VMEM((hid, 2 * hid), BF16),
            pltpu.VMEM((nf,) + result, F32),
            pltpu.VMEM((workers,) + result, F32),
            dma((11,)),
            pltpu.SemaphoreType.REGULAR,
            dma((2,)),
            dma((2, nd // 2)),
            dma((2,)),
            dma((nd // 2 + 1,)),
            dma((6,)),
            dma((5,)),
        ],
        compiler_params=pltpu.CompilerParams(collective_id=0, has_side_effects=True),
    )(
        features,
        seed_rows.reshape(1, seeds),
        want_rows,
        live_counts,
        hop_one,
        hop_two,
        w1_self,
        w1_neigh,
        w2_self.T,
        w2_neigh.T,
        b1.reshape(1, hid_dev),
        b2.reshape(1, hid_dev),
    )


def solution(mesh):
    return jax.shard_map(
        functools.partial(per_device, mesh.shape["dom"], mesh.shape["feat"]),
        mesh=mesh,
        in_specs=(
            P("feat", "dom"),
            P("dom"),
            P("dom", None, None),
            P("dom", None),
            P(None, "dom"),
            P(None, None, "dom"),
            P(),
            P(),
            P("feat"),
            P(None, "feat"),
            P(None, "feat"),
            P("feat"),
        ),
        out_specs=P("feat", "dom"),
        check_vma=False,
    )
```
